32 devices in a mesh: grp: 2 (over y), wide: 8 (over z, x), narrow: 2 (over core).
Axes of the slice: x: 2, y: 2, z: 4, core: 2. Of those that a mesh axis runs over, the one named last changes fastest.
Arguments:
- cache: bfloat16 [16, 48, 576], P('grp', ('wide', 'narrow')), parts along dimension 0, may hold values from -4 to 4
- lengths: int32 [16], P('grp'), parts along dimension 0, may hold values from 1 to 47, 128 in all
- slots: int32 [16], P('grp'), parts along dimension 0, may hold values from 0 to 7, each once
- query: bfloat16 [16, 1, 64, 576], P(('grp', 'wide'), None, 'narrow'), parts along dimension 0, may hold values from -200 to 200
Outputs:
- attended: bfloat16 [16, 1, 64, 512], P(('grp', 'wide'), None, 'narrow'), parts along dimension 0
The draws below stay inside these ranges and needn't reach their ends.
There are 2 independent parts, one for each index of `grp`. The reference program is written for one: setup_inputs(seed, part) draws one part's arguments, and reference() takes and returns one part's arrays. A program takes and returns all parts, laid end to end along the dimension named above; each array names one. Nothing has to cross between parts.
Inputs may be any that keep to these rules, and one draw needn't show every extreme that they name: `lengths`: each request has at most 47 cached positions, and some request has exactly that many in every draw; its 1 new tokens' entries follow its cached positions. `slots`: A permutation: every slot holds one request.
All inputs are finite; a program needn't handle non-finite values.
Results may differ from the reference program's by a relative error of at most 0.013.
Values may be sent and summed in bfloat16 or wider, within the bound.
A program may use at most 64 MiB of HBM per device.

```python
import math
import jax
import jax.numpy as jnp
import numpy as np
from jax import lax

HEAD_TOTAL = 64
LATENT_WIDTH = 512
ROTARY_WIDTH = 64
QUERY_TOKENS = 1
REQUEST_SLOTS = 8
CACHE_POSITIONS = 48


def draw_cache(key, part):
    array_shape = (REQUEST_SLOTS, CACHE_POSITIONS, LATENT_WIDTH + ROTARY_WIDTH)
    value_rows = jnp.clip(jax.random.normal(jax.random.fold_in(key, 3), array_shape, jnp.float32), -4.0, 4.0)
    return value_rows.astype(jnp.bfloat16)


def draw_query(key, part):
    array_shape = (REQUEST_SLOTS, QUERY_TOKENS, HEAD_TOTAL, LATENT_WIDTH + ROTARY_WIDTH)
    value_rows = jnp.clip(0.6 * jax.random.normal(jax.random.fold_in(key, 5), array_shape, jnp.float32), -2.4, 2.4)
    return value_rows.astype(jnp.bfloat16)


def length_profile(count, total, bound, skew):
    loads = [(1 << 20) // math.isqrt(rank ** skew) + 1 for rank in range(2, count + 1)]
    rest, holding = total - bound - (count - 1), [1] * (count - 1)
    while rest > 0:
        free = [i for i in range(count - 1) if holding[i] < bound]
        whole, budget = sum([loads[i] for i in free]), rest
        for i in free:
            extra = min(bound - holding[i], max(1, budget * loads[i] // whole), rest)
            holding[i] = holding[i] + extra
            rest = rest - extra
    return np.array([bound] + holding)


def ragged_sizes(key, count, total, reach, slope):
    if count == 2:
        one = jax.random.randint(key, (), max(1, total - reach), min(reach, total - 1) + 1)
        return jnp.stack([one, total - one])
    sizes = jnp.asarray(length_profile(count, total, reach, slope), jnp.int32)
    couples = (count - 1) // 2
    donor, sink = sizes[1:1 + 2 * couples:2], sizes[2:2 + 2 * couples:2]
    margin = jnp.minimum(donor - 1, reach - sink)
    shifted = jax.random.randint(jax.random.fold_in(key, 1), (couples,), 0, 1 << 20) % (margin + 1)
    sizes = sizes.at[1:1 + 2 * couples:2].set(donor - shifted).at[2:2 + 2 * couples:2].set(sink + shifted)
    return sizes[jax.random.permutation(jax.random.fold_in(key, 2), count)]


def setup_inputs(seed: int = 0, part: int = 0) -> dict:
    seeds = jax.random.split(jax.random.key(seed), 5)
    part_keys = jax.random.split(jax.random.fold_in(seeds[4], part), 5)
    return {
        "cache": draw_cache(jax.random.fold_in(jax.random.fold_in(seeds[4], part), 71), part),
        "lengths": ragged_sizes(part_keys[1], REQUEST_SLOTS, REQUEST_SLOTS * CACHE_POSITIONS // 3, CACHE_POSITIONS - QUERY_TOKENS, 2).astype(jnp.int32),
        "slots": jax.random.permutation(part_keys[2], REQUEST_SLOTS).astype(jnp.int32),
        "query": draw_query(jax.random.fold_in(jax.random.fold_in(seeds[4], part), 71), part),
    }


def reference(cache, lengths, slots, query):
    score_scale = 0.0721687836
    owner = jnp.argsort(slots).astype(jnp.int32)
    positions = jnp.arange(CACHE_POSITIONS, dtype=jnp.int32)
    forward_steps = jnp.arange(QUERY_TOKENS, dtype=jnp.int32)

    def attend(slot_index):
        request = owner[slot_index]
        cache_key_rows = cache[request].astype(jnp.float32)
        query_rows = query[slot_index].astype(jnp.float32)
        scores = jnp.einsum("thc,pc->thp", query_rows, cache_key_rows) * score_scale
        key_limit = lengths[request] + forward_steps + 1
        visible = positions[None, None, :] < key_limit[:, None, None]
        scores = jnp.where(visible, scores, -1.0e30)
        highest = jnp.max(scores, axis=2, keepdims=True)
        softmax_weights = jnp.where(visible, jnp.exp(scores - highest), 0.0)
        weight_sum = jnp.sum(softmax_weights, axis=2)
        rounded_length = lax.optimization_barrier(softmax_weights.astype(jnp.bfloat16)).astype(jnp.float32)
        latent_total = jnp.einsum("seg,gr->ser", rounded_length, cache_key_rows[:, :LATENT_WIDTH])
        return (latent_total / weight_sum[..., None]).astype(jnp.bfloat16)

    return lax.map(attend, jnp.arange(REQUEST_SLOTS, dtype=jnp.int32))
```

```python
import functools

import jax
import jax.numpy as jnp
from jax import lax
from jax.experimental import pallas as pl
from jax.experimental.pallas import tpu as pltpu
from jax.sharding import PartitionSpec as P

LATENT_WIDTH = 512
UNROLL_LIMIT = 16
GROUP_LIMIT = 4
DIRECT_LIMIT = 64

score_scale = 0.0721687836
floor_value = -1e30


def loop(count, body):
    if count <= UNROLL_LIMIT:
        for step in range(count):
            body(step)
    else:
        lax.fori_loop(0, count, lambda step, carry: (body(step), carry)[1], 0)


def kernel(
    wide_count,
    narrow_count,
    direct,
    cache_hbm,
    lengths_hbm,
    slots_hbm,
    query_hbm,
    out_ref,
    cache_ref,
    lengths_ref,
    slots_ref,
    query_ref,
    outgoing,
    received,
    direct_ref,
    local_sem,
    send_sem,
    recv_sem,
    direct_sem,
    arrived_sem,
):
    wide_index = lax.axis_index("wide")
    narrow_index = lax.axis_index("narrow")
    me = wide_index * narrow_count + narrow_index
    peer_count = wide_count * narrow_count
    shard_rows, request_count, channels = cache_ref.shape
    slab_rows = outgoing.shape[1]
    late_source = (wide_count - 1) * narrow_count

    cache_copy = pltpu.make_async_copy(cache_hbm, cache_ref, local_sem.at[1])
    slots_copy = pltpu.make_async_copy(slots_hbm, slots_ref, local_sem.at[0])
    lengths_copy = pltpu.make_async_copy(lengths_hbm, lengths_ref, local_sem.at[2])
    query_copy = pltpu.make_async_copy(query_hbm, query_ref, local_sem.at[3])
    cache_copy.start()
    slots_copy.start()

    def device(index):
        if isinstance(index, int):
            return {"wide": index // narrow_count, "narrow": index % narrow_count}
        return {"wide": lax.div(index, narrow_count), "narrow": lax.rem(index, narrow_count)}

    def signal(semaphore, index):
        pl.semaphore_signal(
            semaphore, inc=1, device_id=device(index), device_id_type=pl.DeviceIdType.MESH
        )

    hub = narrow_count - 1
    is_hub = me == hub
    group_wides = -(-(wide_count - 1) // GROUP_LIMIT)
    group_count = -(-(wide_count - 1) // group_wides)
    group = lax.div(wide_index + group_wides - 1, group_wides) - 1
    barrier = pltpu.get_barrier_semaphore()

    @pl.when((wide_index == 0) & ~is_hub)
    def _():
        signal(barrier, hub)

    pl.semaphore_wait(barrier, jnp.where(is_hub, narrow_count - 1, 1))

    if direct:
        direct_copy = pltpu.make_async_remote_copy(
            src_ref=cache_hbm,
            dst_ref=direct_ref,
            send_sem=direct_sem.at[0],
            recv_sem=direct_sem.at[1],
            device_id={"wide": 0, "narrow": 0},
            device_id_type=pl.DeviceIdType.MESH,
        )

        @pl.when(me == late_source)
        def _():
            direct_copy.start()

    @pl.when(wide_index > 0)
    def _():
        signal(arrived_sem.at[group], hub)

    def announce():
        loop(peer_count - narrow_count, lambda step: signal(barrier, peer_count - 1 - step))
        loop(narrow_count - 1, lambda step: signal(barrier, step))

    pl.when(is_hub)(announce)

    lengths_copy.start()
    query_copy.start()
    slots_copy.wait()
    slot_row = slots_ref[...].reshape(1, request_count)
    shape = (request_count * slab_rows, request_count)
    row = lax.broadcasted_iota(jnp.int32, shape, 0)
    picks = [
        (slot_row * slab_rows + offset == row).astype(jnp.float32).astype(jnp.bfloat16)
        for offset in range(shard_rows)
    ]
    cache_copy.wait()
    ordered = None
    for offset in range(shard_rows):
        term = jnp.dot(picks[offset], cache_ref[offset], preferred_element_type=jnp.float32)
        ordered = term if ordered is None else ordered + term
    outgoing[...] = ordered.reshape(outgoing.shape).astype(jnp.bfloat16)

    def send(index):
        target = device(index)
        wanted = index != me
        if direct and index == 0:
            wanted = wanted & (me != late_source)

        @pl.when(wanted)
        def _():
            pltpu.make_async_remote_copy(
                src_ref=outgoing.at[target["wide"]],
                dst_ref=received.at[me],
                send_sem=send_sem,
                recv_sem=recv_sem,
                device_id=target,
                device_id_type=pl.DeviceIdType.MESH,
            ).start()

    loop(narrow_count, send)
    received[me] = outgoing[wide_index]
    if direct:

        @pl.when(me == 0)
        def _():
            received[late_source] = jnp.zeros(received.shape[1:], received.dtype)

    for step in range(group_count):
        first = (1 + step * group_wides) * narrow_count
        last = min(1 + (step + 1) * group_wides, wide_count) * narrow_count

        @pl.when(is_hub)
        def _():
            pl.semaphore_wait(arrived_sem.at[step], last - first)
            announce()

        @pl.when(~is_hub)
        def _():
            pl.semaphore_wait(barrier, 1)

        loop(last - first, lambda at: send(at + first))

    lengths_copy.wait()
    query_copy.wait()
    own = slot_row == wide_index
    own_length = jnp.sum(
        jnp.where(own, lengths_ref[...].reshape(1, request_count).astype(jnp.float32), 0.0),
        axis=1,
        keepdims=True,
    )
    _, forward_steps, head_count, _ = query_ref.shape
    score_shape = (forward_steps * head_count, peer_count * slab_rows)
    query_rows = query_ref[...].reshape(score_shape[0], channels)
    column = lax.broadcasted_iota(jnp.int32, score_shape, 1)
    offset = column % slab_rows
    source = column // slab_rows
    place = source * shard_rows + offset
    token = lax.broadcasted_iota(jnp.int32, score_shape, 0) // head_count
    visible = (offset < shard_rows) & ((place - token).astype(jnp.float32) < own_length + 1.0)
    if direct:
        visible = visible & ((source != late_source) | (me != 0))
        square = (request_count, request_count)
        diagonal = lax.broadcasted_iota(jnp.int32, square, 0) == lax.broadcasted_iota(
            jnp.int32, square, 1
        )
        own_column = jnp.sum(jnp.where(diagonal & own, 1.0, 0.0), axis=1, keepdims=True)
        query_wide = query_rows.astype(jnp.float32)
        late_token = lax.broadcasted_iota(jnp.int32, (score_shape[0], 1), 0) // head_count
        late_visible = [
            (late_source * shard_rows + at - late_token).astype(jnp.float32) < own_length + 1.0
            for at in range(shard_rows)
        ]

    def wait_slabs(semaphore, spared):
        def wait(count):
            slabs = received.at[pl.ds(0, count)]
            pltpu.make_async_copy(slabs, slabs, semaphore).wait()

        if direct:
            pl.when(me == spared)(lambda: wait(peer_count - 2))
            pl.when(me != spared)(lambda: wait(peer_count - 1))
        else:
            wait(peer_count - 1)

    wait_slabs(recv_sem, 0)

    keys = received[...].reshape(peer_count * slab_rows, channels)
    scores = (
        lax.dot_general(
            query_rows, keys, (((1,), (1,)), ((), ())), preferred_element_type=jnp.float32
        )
        * score_scale
    )
    scores = jnp.where(visible, scores, floor_value)
    highest = jnp.max(scores, axis=1, keepdims=True)
    weights = jnp.where(visible, jnp.exp(scores - highest), 0.0)
    weight_sum = jnp.sum(weights, axis=1, keepdims=True)
    latent_total = jnp.dot(
        weights.astype(jnp.bfloat16), keys[:, :LATENT_WIDTH], preferred_element_type=jnp.float32
    )

    def finish(total, total_weight):
        out_ref[...] = (total / total_weight).astype(jnp.bfloat16).reshape(out_ref.shape)

    if direct:

        @pl.when(me != 0)
        def _():
            finish(latent_total, weight_sum)

        @pl.when(me == 0)
        def _():
            direct_copy.wait_recv()
            late_rows, late_scores, joint = [], [], highest
            for at in range(shard_rows):
                late_row = jnp.sum(
                    direct_ref[at].astype(jnp.float32) * own_column, axis=0, keepdims=True
                )
                score = jnp.sum(query_wide * late_row, axis=1, keepdims=True) * score_scale
                score = jnp.where(late_visible[at], score, floor_value)
                joint = jnp.maximum(joint, score)
                late_rows.append(late_row[:, :LATENT_WIDTH])
                late_scores.append(score)
            scale = jnp.exp(highest - joint)
            total_weight = weight_sum * scale
            total = latent_total * scale
            for at in range(shard_rows):
                weight = jnp.where(late_visible[at], jnp.exp(late_scores[at] - joint), 0.0)
                total_weight = total_weight + weight
                total = total + weight * late_rows[at]
            finish(total, total_weight)
    else:
        finish(latent_total, weight_sum)
    wait_slabs(send_sem, late_source)
    if direct:

        @pl.when(me == late_source)
        def _():
            direct_copy.wait_send()


def padded_bytes(rows, columns):
    return rows * -(-columns // 128) * 128 * 4


def shards(cache, lengths, slots, query):
    wide_count = lax.axis_size("wide")
    narrow_count = lax.axis_size("narrow")
    peer_count = wide_count * narrow_count
    request_count, shard_rows, channels = cache.shape
    _, forward_steps, head_count, _ = query.shape
    slab_rows = pl.next_power_of_2(shard_rows)
    direct = wide_count % 2 == 0 and request_count * shard_rows <= DIRECT_LIMIT
    group_wides = -(-(wide_count - 1) // GROUP_LIMIT)
    group_count = -(-(wide_count - 1) // group_wides)
    slabs = (request_count + peer_count) * slab_rows
    limit = (4 << 20) + 4 * padded_bytes(slabs, channels)
    return pl.pallas_call(
        functools.partial(kernel, wide_count, narrow_count, direct),
        out_shape=jax.ShapeDtypeStruct((1, forward_steps, head_count, LATENT_WIDTH), jnp.bfloat16),
        in_specs=[pl.BlockSpec(memory_space=pltpu.HBM)] * 4,
        out_specs=pl.BlockSpec(memory_space=pltpu.VMEM),
        scratch_shapes=[
            pltpu.VMEM((shard_rows, request_count, channels), cache.dtype),
            pltpu.VMEM(lengths.shape, lengths.dtype),
            pltpu.VMEM(slots.shape, slots.dtype),
            pltpu.VMEM(query.shape, query.dtype),
            pltpu.VMEM((request_count, slab_rows, channels), cache.dtype),
            pltpu.VMEM((peer_count, slab_rows, channels), cache.dtype),
            pltpu.VMEM((shard_rows, request_count, channels), cache.dtype),
            pltpu.SemaphoreType.DMA((4,)),
            pltpu.SemaphoreType.DMA,
            pltpu.SemaphoreType.DMA,
            pltpu.SemaphoreType.DMA((2,)),
            pltpu.SemaphoreType.REGULAR((group_count,)),
        ],
        compiler_params=pltpu.CompilerParams(
            collective_id=0, has_side_effects=True, vmem_limit_bytes=limit
        ),
    )(*[
        pltpu.with_memory_space_constraint(argument, pltpu.HBM)
        for argument in (jnp.transpose(cache, (1, 0, 2)), lengths, slots, query)
    ])


def solution(mesh):
    return jax.shard_map(
        shards,
        mesh=mesh,
        in_specs=(
            P("grp", ("wide", "narrow"), None),
            P("grp"),
            P("grp"),
            P(("grp", "wide"), None, "narrow", None),
        ),
        out_specs=P(("grp", "wide"), None, "narrow", None),
        check_vma=False,
    )
```

```python
import functools

import jax
import jax.numpy as jnp
from jax import lax
from jax.experimental import pallas as pl
from jax.experimental.pallas import tpu as pltpu
from jax.sharding import PartitionSpec as P

LATENT_WIDTH = 512
UNROLL_LIMIT = 16
GROUP_LIMIT = 4
DIRECT_LIMIT = 64

score_scale = 0.0721687836
floor_value = -1e30


def loop(count, body):
    if count <= UNROLL_LIMIT:
        for step in range(count):
            body(step)
    else:
        lax.fori_loop(0, count, lambda step, carry: (body(step), carry)[1], 0)


def kernel(
    wide_count,
    narrow_count,
    direct,
    cache_hbm,
    lengths_hbm,
    slots_hbm,
    query_hbm,
    out_ref,
    cache_ref,
    lengths_ref,
    slots_ref,
    query_ref,
    outgoing,
    received,
    direct_ref,
    late_ref,
    local_sem,
    recv_sem,
    late_sem,
    arrived_sem,
):
    wide_index = lax.axis_index("wide")
    narrow_index = lax.axis_index("narrow")
    me = wide_index * narrow_count + narrow_index
    peer_count = wide_count * narrow_count
    shard_rows, request_count, channels = cache_ref.shape
    slab_rows = outgoing.shape[1]
    late_source = (wide_count - 1) * narrow_count

    cache_copy = pltpu.make_async_copy(cache_hbm, cache_ref, local_sem.at[0])
    send_sem = local_sem.at[0]
    slots_copy = pltpu.make_async_copy(slots_hbm, slots_ref, local_sem.at[1])
    query_copy = pltpu.make_async_copy(query_hbm, query_ref, local_sem.at[1])
    lengths_copy = pltpu.make_async_copy(lengths_hbm, lengths_ref, local_sem.at[1])
    cache_copy.start()
    slots_copy.start()

    def device(index):
        if isinstance(index, int):
            return {"wide": index // narrow_count, "narrow": index % narrow_count}
        return {"wide": lax.div(index, narrow_count), "narrow": lax.rem(index, narrow_count)}

    def signal(semaphore, index):
        pl.semaphore_signal(
            semaphore, inc=1, device_id=device(index), device_id_type=pl.DeviceIdType.MESH
        )

    hub = narrow_count - 1
    is_hub = me == hub
    group_wides = -(-(wide_count - 1) // GROUP_LIMIT)
    group_count = -(-(wide_count - 1) // group_wides)
    group = lax.div(wide_index + group_wides - 1, group_wides) - 1
    barrier = pltpu.get_barrier_semaphore()

    @pl.when((wide_index == 0) & ~is_hub)
    def _():
        signal(barrier, hub)

    pl.semaphore_wait(barrier, jnp.where(is_hub, narrow_count - 1, 1))

    if direct:
        direct_copy = pltpu.make_async_remote_copy(
            src_ref=cache_hbm,
            dst_ref=direct_ref,
            send_sem=late_sem,
            recv_sem=late_sem,
            device_id=device(0),
            device_id_type=pl.DeviceIdType.MESH,
        )
        is_late_source = me == late_source

        @pl.when(is_late_source)
        def _():
            direct_copy.start()

    @pl.when(wide_index > 0)
    def _():
        signal(arrived_sem.at[group], hub)

    def announce():
        loop(peer_count - narrow_count, lambda step: signal(barrier, peer_count - 1 - step))
        loop(narrow_count - 1, lambda step: signal(barrier, step))

    pl.when(is_hub)(announce)

    slots_copy.wait()
    lengths_copy.start()
    slot_row = slots_ref[...].reshape(1, request_count)
    shape = (request_count * slab_rows, shard_rows * request_count)
    slot_tiled = jnp.concatenate([slot_row] * shard_rows, axis=1)
    row = lax.broadcasted_iota(jnp.int32, shape, 0)
    column = lax.broadcasted_iota(jnp.int32, shape, 1)
    pick = (slot_tiled * slab_rows + lax.div(column, request_count) == row).astype(jnp.float32)
    pick = pick.astype(jnp.bfloat16)
    cache_copy.wait()
    shard = cache_ref[...].reshape(shard_rows * request_count, channels)
    ordered = jnp.dot(pick, shard, preferred_element_type=jnp.float32)
    outgoing[...] = ordered.astype(jnp.bfloat16).reshape(outgoing.shape)

    def send(index, target_ref, target_sem, wanted):
        target = device(index)

        @pl.when(wanted)
        def _():
            pltpu.make_async_remote_copy(
                src_ref=outgoing.at[target["wide"]],
                dst_ref=target_ref,
                send_sem=send_sem,
                recv_sem=target_sem,
                device_id=target,
                device_id_type=pl.DeviceIdType.MESH,
            ).start()

    def send_slab(index, wanted=True):
        send(index, received.at[me], recv_sem, (index != me) & wanted)

    for core in range(narrow_count):
        if direct:
            send_slab(core, ~is_late_source)
            if core > 0:
                send(core, late_ref, late_sem, is_late_source)
        else:
            send_slab(core)
    lengths_copy.wait()
    query_copy.start()
    received[me] = outgoing[wide_index]
    if direct:

        @pl.when(wide_index == 0)
        def _():
            received[late_source] = jnp.zeros(received.shape[1:], received.dtype)

    for step in range(group_count):
        first = (1 + step * group_wides) * narrow_count
        last = min(1 + (step + 1) * group_wides, wide_count) * narrow_count

        @pl.when(is_hub)
        def _():
            pl.semaphore_wait(arrived_sem.at[step], last - first)
            announce()

        @pl.when(~is_hub)
        def _():
            pl.semaphore_wait(barrier, 1)

        loop(last - first, lambda at: send_slab(at + first))

    query_copy.wait()
    own = slot_row == wide_index
    own_length = jnp.sum(
        jnp.where(own, lengths_ref[...].reshape(1, request_count).astype(jnp.float32), 0.0),
        axis=1,
        keepdims=True,
    )
    _, forward_steps, head_count, _ = query_ref.shape
    score_shape = (forward_steps * head_count, peer_count * slab_rows)
    query_rows = query_ref[...].reshape(score_shape[0], channels)
    column = lax.broadcasted_iota(jnp.int32, score_shape, 1)
    offset = column % slab_rows
    source = column // slab_rows
    place = source * shard_rows + offset
    token = lax.broadcasted_iota(jnp.int32, score_shape, 0) // head_count
    visible = (offset < shard_rows) & ((place - token).astype(jnp.float32) < own_length + 1.0)
    if direct:
        visible = visible & ((source != late_source) | (wide_index != 0))
        square = (request_count, request_count)
        diagonal = lax.broadcasted_iota(jnp.int32, square, 0) == lax.broadcasted_iota(
            jnp.int32, square, 1
        )
        own_column = jnp.sum(jnp.where(diagonal & own, 1.0, 0.0), axis=1, keepdims=True)
        query_wide = query_rows.astype(jnp.float32) * score_scale
        late_token = lax.broadcasted_iota(jnp.int32, (score_shape[0], 1), 0) // head_count
        late_visible = [
            (late_source * shard_rows + at - late_token).astype(jnp.float32) < own_length + 1.0
            for at in range(shard_rows)
        ]

    def wait_slabs(semaphore, one_fewer):
        def wait(count):
            slabs = received.at[pl.ds(0, count)]
            pltpu.make_async_copy(slabs, slabs, semaphore).wait()

        if direct:
            pl.when(one_fewer)(lambda: wait(peer_count - 2))
            pl.when(~one_fewer)(lambda: wait(peer_count - 1))
        else:
            wait(peer_count - 1)

    wait_slabs(recv_sem, wide_index == 0)

    keys = received[...].reshape(peer_count * slab_rows, channels)
    scores = (
        lax.dot_general(
            query_rows, keys, (((1,), (1,)), ((), ())), preferred_element_type=jnp.float32
        )
        * score_scale
    )
    scores = jnp.where(visible, scores, floor_value)
    highest = jnp.max(scores, axis=1, keepdims=True)
    weights = jnp.where(visible, jnp.exp(scores - highest), 0.0)
    weight_sum = jnp.sum(weights, axis=1, keepdims=True)
    latent_total = jnp.dot(
        weights.astype(jnp.bfloat16), keys[:, :LATENT_WIDTH], preferred_element_type=jnp.float32
    )

    def finish(total, total_weight):
        out_ref[...] = (total / total_weight).astype(jnp.bfloat16).reshape(out_ref.shape)

    if direct:

        @pl.when(wide_index != 0)
        def _():
            finish(latent_total, weight_sum)

        def fold(late_rows):
            late_scores, joint = [], highest
            for at in range(shard_rows):
                score = jnp.sum(query_wide * late_rows[at], axis=1, keepdims=True)
                score = jnp.where(late_visible[at], score, floor_value)
                joint = jnp.maximum(joint, score)
                late_scores.append(score)
            scale = jnp.exp(highest - joint)
            total_weight = weight_sum * scale
            total = latent_total * scale
            for at in range(shard_rows):
                weight = jnp.where(late_visible[at], jnp.exp(late_scores[at] - joint), 0.0)
                total_weight = total_weight + weight
                total = total + weight * late_rows[at][:, :LATENT_WIDTH]
            finish(total, total_weight)

        @pl.when(me == 0)
        def _():
            direct_copy.wait_recv()
            fold([
                jnp.sum(direct_ref[at].astype(jnp.float32) * own_column, axis=0, keepdims=True)
                for at in range(shard_rows)
            ])

        @pl.when((wide_index == 0) & (me != 0))
        def _():
            pltpu.make_async_copy(late_ref, late_ref, late_sem).wait()
            late_slab = late_ref[...].astype(jnp.float32)
            fold([late_slab[at : at + 1] for at in range(shard_rows)])
    else:
        finish(latent_total, weight_sum)
    wait_slabs(send_sem, is_late_source if direct else False)
    if direct:

        @pl.when(is_late_source)
        def _():
            direct_copy.wait_send()


def padded_bytes(rows, columns):
    return rows * -(-columns // 128) * 128 * 4


def shards(cache, lengths, slots, query):
    wide_count = lax.axis_size("wide")
    narrow_count = lax.axis_size("narrow")
    peer_count = wide_count * narrow_count
    request_count, shard_rows, channels = cache.shape
    _, forward_steps, head_count, _ = query.shape
    slab_rows = pl.next_power_of_2(shard_rows)
    direct = wide_count % 2 == 0 and request_count * shard_rows <= DIRECT_LIMIT
    group_wides = -(-(wide_count - 1) // GROUP_LIMIT)
    group_count = -(-(wide_count - 1) // group_wides)
    slabs = (request_count + peer_count) * slab_rows
    limit = (4 << 20) + 4 * padded_bytes(slabs, channels)
    return pl.pallas_call(
        functools.partial(kernel, wide_count, narrow_count, direct),
        out_shape=jax.ShapeDtypeStruct((1, forward_steps, head_count, LATENT_WIDTH), jnp.bfloat16),
        in_specs=[pl.BlockSpec(memory_space=pltpu.HBM)] * 4,
        out_specs=pl.BlockSpec(memory_space=pltpu.VMEM),
        scratch_shapes=[
            pltpu.VMEM((shard_rows, request_count, channels), cache.dtype),
            pltpu.VMEM(lengths.shape, lengths.dtype),
            pltpu.VMEM(slots.shape, slots.dtype),
            pltpu.VMEM(query.shape, query.dtype),
            pltpu.VMEM((request_count, slab_rows, channels), cache.dtype),
            pltpu.VMEM((peer_count, slab_rows, channels), cache.dtype),
            pltpu.VMEM((shard_rows, request_count, channels), cache.dtype),
            pltpu.VMEM((slab_rows, channels), cache.dtype),
            pltpu.SemaphoreType.DMA((2,)),
            pltpu.SemaphoreType.DMA,
            pltpu.SemaphoreType.DMA,
            pltpu.SemaphoreType.REGULAR((group_count,)),
        ],
        compiler_params=pltpu.CompilerParams(
            collective_id=0, has_side_effects=True, vmem_limit_bytes=limit
        ),
    )(*[
        pltpu.with_memory_space_constraint(argument, pltpu.HBM)
        for argument in (jnp.transpose(cache, (1, 0, 2)), lengths, slots, query)
    ])


def solution(mesh):
    return jax.shard_map(
        shards,
        mesh=mesh,
        in_specs=(
            P("grp", ("wide", "narrow"), None),
            P("grp"),
            P("grp"),
            P(("grp", "wide"), None, "narrow", None),
        ),
        out_specs=P(("grp", "wide"), None, "narrow", None),
        check_vma=False,
    )
```

```python
import functools
import math

import jax
import jax.numpy as jnp
from jax import lax
from jax.experimental import pallas as pl
from jax.experimental.pallas import tpu as pltpu
from jax.sharding import PartitionSpec as P

LATENT_WIDTH = 512
UNROLL_LIMIT = 16
GROUP_LIMIT = 4
DIRECT_LIMIT = 64

score_scale = 0.0721687836
floor_value = -1e30


def loop(count, body):
    if count <= UNROLL_LIMIT:
        for step in range(count):
            body(step)
    else:
        lax.fori_loop(0, count, lambda step, carry: (body(step), carry)[1], 0)


def kernel(
    wide_count,
    narrow_count,
    direct,
    cache_hbm,
    lengths_hbm,
    slots_hbm,
    query_hbm,
    out_ref,
    cache_ref,
    lengths_ref,
    slots_ref,
    query_ref,
    outgoing,
    received,
    direct_ref,
    late_ref,
    local_sem,
    recv_sem,
    late_sem,
    arrived_sem,
):
    wide_index = lax.axis_index("wide")
    narrow_index = lax.axis_index("narrow")
    me = wide_index * narrow_count + narrow_index
    peer_count = wide_count * narrow_count
    shard_rows, request_count, channels = cache_ref.shape
    slab_rows = outgoing.shape[1]
    late_source = (wide_count - 1) * narrow_count

    cache_copy = pltpu.make_async_copy(cache_hbm, cache_ref, local_sem.at[0])
    send_sem = local_sem.at[0]
    slots_copy = pltpu.make_async_copy(slots_hbm, slots_ref, local_sem.at[1])
    query_copy = pltpu.make_async_copy(query_hbm, query_ref, local_sem.at[1])
    lengths_copy = pltpu.make_async_copy(lengths_hbm, lengths_ref, local_sem.at[1])

    def device(index):
        if isinstance(index, int):
            return {"wide": index // narrow_count, "narrow": index % narrow_count}
        return {"wide": lax.div(index, narrow_count), "narrow": lax.rem(index, narrow_count)}

    def signal(semaphore, index):
        pl.semaphore_signal(
            semaphore, inc=1, device_id=device(index), device_id_type=pl.DeviceIdType.MESH
        )

    hub = narrow_count - 1
    is_hub = me == hub
    group_wides = -(-(wide_count - 1) // GROUP_LIMIT)
    group_count = -(-(wide_count - 1) // group_wides)
    group = lax.div(wide_index + group_wides - 1, group_wides) - 1
    barrier = pltpu.get_barrier_semaphore()

    @pl.when((wide_index == 0) & ~is_hub)
    def _():
        signal(barrier, hub)

    pl.semaphore_wait(barrier, jnp.where(is_hub, narrow_count - 1, 1))

    if direct:
        direct_copy = pltpu.make_async_remote_copy(
            src_ref=cache_hbm,
            dst_ref=direct_ref,
            send_sem=late_sem,
            recv_sem=late_sem,
            device_id=device(0),
            device_id_type=pl.DeviceIdType.MESH,
        )
        is_late_source = me == late_source

        @pl.when(is_late_source)
        def _():
            direct_copy.start()

    cache_copy.start()
    slots_copy.start()

    @pl.when(wide_index > 0)
    def _():
        signal(arrived_sem.at[group], hub)

    def announce():
        loop(peer_count - narrow_count, lambda step: signal(barrier, peer_count - 1 - step))
        loop(narrow_count - 1, lambda step: signal(barrier, step))

    pl.when(is_hub)(announce)

    slots_copy.wait()
    lengths_copy.start()
    slot_row = slots_ref[...].reshape(1, request_count)
    shape = (request_count * slab_rows, shard_rows * request_count)
    slot_tiled = jnp.concatenate([slot_row] * shard_rows, axis=1)
    row = lax.broadcasted_iota(jnp.int32, shape, 0)
    column = lax.broadcasted_iota(jnp.int32, shape, 1)
    pick = (slot_tiled * slab_rows + lax.div(column, request_count) == row).astype(jnp.float32)
    pick = pick.astype(jnp.bfloat16)
    cache_copy.wait()
    shard = cache_ref[...].reshape(shard_rows * request_count, channels)
    ordered = jnp.dot(pick, shard, preferred_element_type=jnp.float32)
    outgoing[...] = ordered.astype(jnp.bfloat16).reshape(outgoing.shape)

    def send(index, target_ref, target_sem, wanted):
        target = device(index)

        @pl.when(wanted)
        def _():
            pltpu.make_async_remote_copy(
                src_ref=outgoing.at[target["wide"]],
                dst_ref=target_ref,
                send_sem=send_sem,
                recv_sem=target_sem,
                device_id=target,
                device_id_type=pl.DeviceIdType.MESH,
            ).start()

    def send_slab(index, wanted=True):
        send(index, received.at[me], recv_sem, (index != me) & wanted)

    for core in range(narrow_count):
        if direct:
            send_slab(core, ~is_late_source)
            if core > 0:
                send(core, late_ref, late_sem, is_late_source)
        else:
            send_slab(core)
    lengths_copy.wait()
    query_copy.start()
    received[me] = outgoing[wide_index]
    if direct:

        @pl.when(wide_index == 0)
        def _():
            received[late_source] = jnp.zeros(received.shape[1:], received.dtype)

    for step in range(group_count):
        first = (1 + step * group_wides) * narrow_count
        last = min(1 + (step + 1) * group_wides, wide_count) * narrow_count

        @pl.when(is_hub)
        def _():
            pl.semaphore_wait(arrived_sem.at[step], last - first)
            announce()

        @pl.when(~is_hub)
        def _():
            pl.semaphore_wait(barrier, 1)

        loop(last - first, lambda at: send_slab(at + first))

    query_copy.wait()
    own = slot_row == wide_index
    own_length = jnp.sum(
        jnp.where(own, lengths_ref[...].reshape(1, request_count).astype(jnp.float32), 0.0),
        axis=1,
        keepdims=True,
    )
    _, forward_steps, head_count, _ = query_ref.shape
    tile_heads = math.gcd(head_count, 8)
    score_shape = (forward_steps * head_count, peer_count * slab_rows)
    query_rows = query_ref[...].reshape(score_shape[0], channels)
    column = lax.broadcasted_iota(jnp.int32, score_shape, 1)
    offset = column % slab_rows
    source = column // slab_rows
    place = source * shard_rows + offset
    token = lax.broadcasted_iota(jnp.int32, score_shape, 0) // head_count
    visible = (offset < shard_rows) & ((place - token).astype(jnp.float32) < own_length + 1.0)
    if direct:
        visible = visible & ((source != late_source) | (wide_index != 0))
        square = (request_count, request_count)
        diagonal = lax.broadcasted_iota(jnp.int32, square, 0) == lax.broadcasted_iota(
            jnp.int32, square, 1
        )
        own_column = jnp.sum(jnp.where(diagonal & own, 1.0, 0.0), axis=1, keepdims=True)
        query_wide = query_rows.astype(jnp.float32) * score_scale
        late_token = lax.broadcasted_iota(jnp.int32, (score_shape[0], 1), 0) // head_count
        late_visible = [
            (late_source * shard_rows + at - late_token).astype(jnp.float32) < own_length + 1.0
            for at in range(shard_rows)
        ]

    def wait_slabs(semaphore, one_fewer):
        def wait(count):
            slabs = received.at[pl.ds(0, count)]
            pltpu.make_async_copy(slabs, slabs, semaphore).wait()

        if direct:
            pl.when(one_fewer)(lambda: wait(peer_count - 2))
            pl.when(~one_fewer)(lambda: wait(peer_count - 1))
        else:
            wait(peer_count - 1)

    wait_slabs(recv_sem, wide_index == 0)

    keys = received[...].reshape(peer_count * slab_rows, channels)
    scores = (
        lax.dot_general(
            query_rows, keys, (((1,), (1,)), ((), ())), preferred_element_type=jnp.float32
        )
        * score_scale
    )
    scores = jnp.where(visible, scores, floor_value)
    highest = jnp.max(scores, axis=1, keepdims=True)
    weights = jnp.where(visible, jnp.exp(scores - highest), 0.0)
    weight_sum = jnp.sum(weights, axis=1, keepdims=True)
    latent_total = jnp.dot(
        weights.astype(jnp.bfloat16), keys[:, :LATENT_WIDTH], preferred_element_type=jnp.float32
    )

    def finish(total, total_weight):
        out_ref[...] = (total / total_weight).astype(jnp.bfloat16).reshape(out_ref.shape)

    if direct:

        @pl.when(wide_index != 0)
        def _():
            finish(latent_total, weight_sum)

        def fold(late_rows):
            for token in range(forward_steps):
                for head in range(0, head_count, tile_heads):
                    rows = slice(token * head_count + head, token * head_count + head + tile_heads)
                    late_scores, joint = [], highest[rows]
                    for at in range(shard_rows):
                        score = jnp.sum(query_wide[rows] * late_rows[at], axis=1, keepdims=True)
                        score = jnp.where(late_visible[at][rows], score, floor_value)
                        joint = jnp.maximum(joint, score)
                        late_scores.append(score)
                    scale = jnp.exp(highest[rows] - joint)
                    total_weight = weight_sum[rows] * scale
                    total = latent_total[rows] * scale
                    for at in range(shard_rows):
                        weight = jnp.exp(late_scores[at] - joint)
                        weight = jnp.where(late_visible[at][rows], weight, 0.0)
                        total_weight = total_weight + weight
                        total = total + weight * late_rows[at][:, :LATENT_WIDTH]
                    attended = (total / total_weight).astype(jnp.bfloat16)
                    out_ref[0, token, head : head + tile_heads, :] = attended

        @pl.when(me == 0)
        def _():
            direct_copy.wait_recv()
            fold([
                jnp.sum(direct_ref[at].astype(jnp.float32) * own_column, axis=0, keepdims=True)
                for at in range(shard_rows)
            ])

        @pl.when((wide_index == 0) & (me != 0))
        def _():
            pltpu.make_async_copy(late_ref, late_ref, late_sem).wait()
            late_slab = late_ref[...].astype(jnp.float32)
            fold([late_slab[at : at + 1] for at in range(shard_rows)])
    else:
        finish(latent_total, weight_sum)
    wait_slabs(send_sem, is_late_source if direct else False)
    if direct:

        @pl.when(is_late_source)
        def _():
            direct_copy.wait_send()


def padded_bytes(rows, columns):
    return rows * -(-columns // 128) * 128 * 4


def shards(cache, lengths, slots, query):
    wide_count = lax.axis_size("wide")
    narrow_count = lax.axis_size("narrow")
    peer_count = wide_count * narrow_count
    request_count, shard_rows, channels = cache.shape
    _, forward_steps, head_count, _ = query.shape
    slab_rows = pl.next_power_of_2(shard_rows)
    direct = wide_count % 2 == 0 and request_count * shard_rows <= DIRECT_LIMIT
    group_wides = -(-(wide_count - 1) // GROUP_LIMIT)
    group_count = -(-(wide_count - 1) // group_wides)
    slabs = (request_count + peer_count) * slab_rows
    limit = (4 << 20) + 4 * padded_bytes(slabs, channels)
    return pl.pallas_call(
        functools.partial(kernel, wide_count, narrow_count, direct),
        out_shape=jax.ShapeDtypeStruct((1, forward_steps, head_count, LATENT_WIDTH), jnp.bfloat16),
        in_specs=[pl.BlockSpec(memory_space=pltpu.HBM)] * 4,
        out_specs=pl.BlockSpec(memory_space=pltpu.VMEM),
        scratch_shapes=[
            pltpu.VMEM((shard_rows, request_count, channels), cache.dtype),
            pltpu.VMEM(lengths.shape, lengths.dtype),
            pltpu.VMEM(slots.shape, slots.dtype),
            pltpu.VMEM(query.shape, query.dtype),
            pltpu.VMEM((request_count, slab_rows, channels), cache.dtype),
            pltpu.VMEM((peer_count, slab_rows, channels), cache.dtype),
            pltpu.VMEM((shard_rows, request_count, channels), cache.dtype),
            pltpu.VMEM((slab_rows, channels), cache.dtype),
            pltpu.SemaphoreType.DMA((2,)),
            pltpu.SemaphoreType.DMA,
            pltpu.SemaphoreType.DMA,
            pltpu.SemaphoreType.REGULAR((group_count,)),
        ],
        compiler_params=pltpu.CompilerParams(
            collective_id=0, has_side_effects=True, vmem_limit_bytes=limit
        ),
    )(*[
        pltpu.with_memory_space_constraint(argument, pltpu.HBM)
        for argument in (jnp.transpose(cache, (1, 0, 2)), lengths, slots, query)
    ])


def solution(mesh):
    return jax.shard_map(
        shards,
        mesh=mesh,
        in_specs=(
            P("grp", ("wide", "narrow"), None),
            P("grp"),
            P("grp"),
            P(("grp", "wide"), None, "narrow", None),
        ),
        out_specs=P(("grp", "wide"), None, "narrow", None),
        check_vma=False,
    )
```

```python
import functools
import math

import jax
import jax.numpy as jnp
from jax import lax
from jax.experimental import pallas as pl
from jax.experimental.pallas import tpu as pltpu
from jax.sharding import PartitionSpec as P

LATENT_WIDTH = 512
UNROLL_LIMIT = 16
GROUP_LIMIT = 4
DIRECT_LIMIT = 64

score_scale = 0.0721687836 * math.log2(math.e)
floor_value = -1e30


def loop(count, body):
    if count <= UNROLL_LIMIT:
        for step in range(count):
            body(step)
    else:
        lax.fori_loop(0, count, lambda step, carry: (body(step), carry)[1], 0)


def kernel(
    wide_count,
    narrow_count,
    direct,
    cache_hbm,
    lengths_hbm,
    slots_hbm,
    query_hbm,
    out_ref,
    cache_ref,
    lengths_ref,
    slots_ref,
    query_ref,
    outgoing,
    received,
    direct_ref,
    late_ref,
    local_sem,
    recv_sem,
    late_sem,
    arrived_sem,
):
    wide_index = lax.axis_index("wide")
    narrow_index = lax.axis_index("narrow")
    me = wide_index * narrow_count + narrow_index
    peer_count = wide_count * narrow_count
    shard_rows, request_count, channels = cache_ref.shape
    slab_rows = outgoing.shape[1]
    late_source = (wide_count - 1) * narrow_count

    cache_copy = pltpu.make_async_copy(cache_hbm, cache_ref, local_sem.at[0])
    send_sem = local_sem.at[0]
    slots_copy = pltpu.make_async_copy(slots_hbm, slots_ref, local_sem.at[1])
    query_copy = pltpu.make_async_copy(query_hbm, query_ref, local_sem.at[1])
    lengths_copy = pltpu.make_async_copy(lengths_hbm, lengths_ref, local_sem.at[1])

    def device(index):
        if isinstance(index, int):
            return {"wide": index // narrow_count, "narrow": index % narrow_count}
        return {"wide": lax.div(index, narrow_count), "narrow": lax.rem(index, narrow_count)}

    def signal(semaphore, index):
        pl.semaphore_signal(
            semaphore, inc=1, device_id=device(index), device_id_type=pl.DeviceIdType.MESH
        )

    hub = narrow_count - 1
    is_hub = me == hub
    group_wides = -(-(wide_count - 1) // GROUP_LIMIT)
    group_count = -(-(wide_count - 1) // group_wides)
    group = lax.div(wide_index + group_wides - 1, group_wides) - 1
    barrier = pltpu.get_barrier_semaphore()

    @pl.when((wide_index == 0) & ~is_hub)
    def _():
        signal(barrier, hub)

    pl.semaphore_wait(barrier, jnp.where(is_hub, narrow_count - 1, 1))

    if direct:
        direct_copy = pltpu.make_async_remote_copy(
            src_ref=cache_hbm,
            dst_ref=direct_ref,
            send_sem=late_sem,
            recv_sem=late_sem,
            device_id=device(0),
            device_id_type=pl.DeviceIdType.MESH,
        )
        is_late_source = me == late_source

        @pl.when(is_late_source)
        def _():
            direct_copy.start()

    cache_copy.start()
    slots_copy.start()

    @pl.when(group == 0)
    def _():
        signal(barrier, hub)

    @pl.when(group > 0)
    def _():
        signal(arrived_sem.at[group - 1], hub)

    def announce():
        loop(peer_count - narrow_count, lambda step: signal(barrier, peer_count - 1 - step))
        loop(narrow_count - 1, lambda step: signal(barrier, step))

    pl.when(is_hub)(announce)

    slots_copy.wait()
    lengths_copy.start()
    slot_row = slots_ref[...].reshape(1, request_count)
    shape = (request_count * slab_rows, shard_rows * request_count)
    slot_tiled = jnp.concatenate([slot_row] * shard_rows, axis=1)
    row = lax.broadcasted_iota(jnp.int32, shape, 0)
    column = lax.broadcasted_iota(jnp.int32, shape, 1)
    pick = (slot_tiled * slab_rows + lax.div(column, request_count) == row).astype(jnp.float32)
    pick = pick.astype(jnp.bfloat16)
    cache_copy.wait()
    shard = cache_ref[...].reshape(shard_rows * request_count, channels)
    ordered = jnp.dot(pick, shard, preferred_element_type=jnp.float32)
    outgoing[...] = ordered.astype(jnp.bfloat16).reshape(outgoing.shape)

    def send(index, target_ref, target_sem, wanted):
        target = device(index)

        @pl.when(wanted)
        def _():
            pltpu.make_async_remote_copy(
                src_ref=outgoing.at[target["wide"]],
                dst_ref=target_ref,
                send_sem=send_sem,
                recv_sem=target_sem,
                device_id=target,
                device_id_type=pl.DeviceIdType.MESH,
            ).start()

    def send_slab(index, wanted=True):
        send(index, received.at[me], recv_sem, (index != me) & wanted)

    for core in range(narrow_count):
        if direct:
            send_slab(core, ~is_late_source)
            if core > 0:
                send(core, late_ref, late_sem, is_late_source)
        else:
            send_slab(core)
    lengths_copy.wait()
    query_copy.start()
    received[me] = outgoing[wide_index]
    if direct:

        @pl.when(wide_index == 0)
        def _():
            received[late_source] = jnp.zeros(received.shape[1:], received.dtype)

    for step in range(group_count):
        first = (1 + step * group_wides) * narrow_count
        last = min(1 + (step + 1) * group_wides, wide_count) * narrow_count

        @pl.when(is_hub)
        def _():
            answered = barrier if step == 0 else arrived_sem.at[step - 1]
            pl.semaphore_wait(answered, last - first)
            announce()

        @pl.when(~is_hub)
        def _():
            pl.semaphore_wait(barrier, 1)

        loop(last - first, lambda at: send_slab(at + first))

    query_copy.wait()
    own = slot_row == wide_index
    own_length = jnp.sum(
        jnp.where(own, lengths_ref[...].reshape(1, request_count).astype(jnp.float32), 0.0),
        axis=1,
        keepdims=True,
    )
    _, forward_steps, head_count, _ = query_ref.shape
    tile_heads = math.gcd(head_count, 8)
    score_shape = (forward_steps * head_count, peer_count * slab_rows)
    query_rows = query_ref[...].reshape(score_shape[0], channels)
    column = lax.broadcasted_iota(jnp.int32, score_shape, 1)
    offset = column % slab_rows
    source = column // slab_rows
    place = source * shard_rows + offset
    token = lax.broadcasted_iota(jnp.int32, score_shape, 0) // head_count
    visible = (offset < shard_rows) & ((place - token).astype(jnp.float32) < own_length + 1.0)
    if direct:
        visible = visible & ((source != late_source) | (wide_index != 0))
        square = (request_count, request_count)
        diagonal = lax.broadcasted_iota(jnp.int32, square, 0) == lax.broadcasted_iota(
            jnp.int32, square, 1
        )
        own_column = jnp.sum(jnp.where(diagonal & own, 1.0, 0.0), axis=1, keepdims=True)
        query_wide = query_rows.astype(jnp.float32) * score_scale
        late_token = lax.broadcasted_iota(jnp.int32, (score_shape[0], 1), 0) // head_count
        late_visible = [
            (late_source * shard_rows + at - late_token).astype(jnp.float32) < own_length + 1.0
            for at in range(shard_rows)
        ]

    def wait_slabs(semaphore, one_fewer):
        def wait(count):
            slabs = received.at[pl.ds(0, count)]
            pltpu.make_async_copy(slabs, slabs, semaphore).wait()

        if direct:
            pl.when(one_fewer)(lambda: wait(peer_count - 2))
            pl.when(~one_fewer)(lambda: wait(peer_count - 1))
        else:
            wait(peer_count - 1)

    wait_slabs(recv_sem, wide_index == 0)

    keys = received[...].reshape(peer_count * slab_rows, channels)
    scores = (
        lax.dot_general(
            query_rows, keys, (((1,), (1,)), ((), ())), preferred_element_type=jnp.float32
        )
        * score_scale
    )
    scores = jnp.where(visible, scores, floor_value)
    highest = jnp.max(scores, axis=1, keepdims=True)
    weights = jnp.exp2(scores - highest)
    weight_sum = jnp.sum(weights, axis=1, keepdims=True)
    latent_total = jnp.dot(
        weights.astype(jnp.bfloat16), keys[:, :LATENT_WIDTH], preferred_element_type=jnp.float32
    )

    def finish(total, total_weight):
        out_ref[...] = (total / total_weight).astype(jnp.bfloat16).reshape(out_ref.shape)

    if direct:

        @pl.when(wide_index != 0)
        def _():
            finish(latent_total, weight_sum)

        def fold(late_rows):
            for token in range(forward_steps):
                for head in range(0, head_count, tile_heads):
                    rows = slice(token * head_count + head, token * head_count + head + tile_heads)
                    late_scores, joint = [], highest[rows]
                    for at in range(shard_rows):
                        score = jnp.sum(query_wide[rows] * late_rows[at], axis=1, keepdims=True)
                        score = jnp.where(late_visible[at][rows], score, floor_value)
                        joint = jnp.maximum(joint, score)
                        late_scores.append(score)
                    scale = jnp.exp2(highest[rows] - joint)
                    total_weight = weight_sum[rows] * scale
                    total = latent_total[rows] * scale
                    for at in range(shard_rows):
                        weight = jnp.exp2(late_scores[at] - joint)
                        total_weight = total_weight + weight
                        total = total + weight * late_rows[at][:, :LATENT_WIDTH]
                    attended = (total / total_weight).astype(jnp.bfloat16)
                    out_ref[0, token, head : head + tile_heads, :] = attended

        @pl.when(me == 0)
        def _():
            direct_copy.wait_recv()
            fold([
                jnp.sum(direct_ref[at].astype(jnp.float32) * own_column, axis=0, keepdims=True)
                for at in range(shard_rows)
            ])

        @pl.when((wide_index == 0) & (me != 0))
        def _():
            pltpu.make_async_copy(late_ref, late_ref, late_sem).wait()
            late_slab = late_ref[...].astype(jnp.float32)
            fold([late_slab[at : at + 1] for at in range(shard_rows)])
    else:
        finish(latent_total, weight_sum)
    wait_slabs(send_sem, is_late_source if direct else False)
    if direct:

        @pl.when(is_late_source)
        def _():
            direct_copy.wait_send()


def padded_bytes(rows, columns):
    return rows * -(-columns // 128) * 128 * 4


def shards(cache, lengths, slots, query):
    wide_count = lax.axis_size("wide")
    narrow_count = lax.axis_size("narrow")
    peer_count = wide_count * narrow_count
    request_count, shard_rows, channels = cache.shape
    _, forward_steps, head_count, _ = query.shape
    slab_rows = pl.next_power_of_2(shard_rows)
    direct = wide_count % 2 == 0 and request_count * shard_rows <= DIRECT_LIMIT
    group_wides = -(-(wide_count - 1) // GROUP_LIMIT)
    group_count = -(-(wide_count - 1) // group_wides)
    slabs = (request_count + peer_count) * slab_rows
    limit = (4 << 20) + 4 * padded_bytes(slabs, channels)
    return pl.pallas_call(
        functools.partial(kernel, wide_count, narrow_count, direct),
        out_shape=jax.ShapeDtypeStruct((1, forward_steps, head_count, LATENT_WIDTH), jnp.bfloat16),
        in_specs=[pl.BlockSpec(memory_space=pltpu.HBM)] * 4,
        out_specs=pl.BlockSpec(memory_space=pltpu.VMEM),
        scratch_shapes=[
            pltpu.VMEM((shard_rows, request_count, channels), cache.dtype),
            pltpu.VMEM(lengths.shape, lengths.dtype),
            pltpu.VMEM(slots.shape, slots.dtype),
            pltpu.VMEM(query.shape, query.dtype),
            pltpu.VMEM((request_count, slab_rows, channels), cache.dtype),
            pltpu.VMEM((peer_count, slab_rows, channels), cache.dtype),
            pltpu.VMEM((shard_rows, request_count, channels), cache.dtype),
            pltpu.VMEM((slab_rows, channels), cache.dtype),
            pltpu.SemaphoreType.DMA((2,)),
            pltpu.SemaphoreType.DMA,
            pltpu.SemaphoreType.DMA,
            pltpu.SemaphoreType.REGULAR((max(group_count - 1, 1),)),
        ],
        compiler_params=pltpu.CompilerParams(
            collective_id=0, has_side_effects=True, vmem_limit_bytes=limit
        ),
    )(*[
        pltpu.with_memory_space_constraint(argument, pltpu.HBM)
        for argument in (jnp.transpose(cache, (1, 0, 2)), lengths, slots, query)
    ])


def solution(mesh):
    return jax.shard_map(
        shards,
        mesh=mesh,
        in_specs=(
            P("grp", ("wide", "narrow"), None),
            P("grp"),
            P("grp"),
            P(("grp", "wide"), None, "narrow", None),
        ),
        out_specs=P(("grp", "wide"), None, "narrow", None),
        check_vma=False,
    )
```

```python
import functools
import math

import jax
import jax.numpy as jnp
from jax import lax
from jax.experimental import pallas as pl
from jax.experimental.pallas import tpu as pltpu
from jax.sharding import PartitionSpec as P

LATENT_WIDTH = 512
UNROLL_LIMIT = 16
GROUP_LIMIT = 4
DIRECT_LIMIT = 64

score_scale = 0.0721687836 * math.log2(math.e)
floor_value = -1e30


def loop(count, body):
    if count <= UNROLL_LIMIT:
        for step in range(count):
            body(step)
    else:
        lax.fori_loop(0, count, lambda step, carry: (body(step), carry)[1], 0)


def kernel(
    wide_count,
    narrow_count,
    direct,
    cache_hbm,
    lengths_hbm,
    slots_hbm,
    query_hbm,
    out_ref,
    cache_ref,
    lengths_ref,
    slots_ref,
    query_ref,
    outgoing,
    received,
    direct_ref,
    late_ref,
    local_sem,
    recv_sem,
    late_sem,
    arrived_sem,
):
    wide_index = lax.axis_index("wide")
    narrow_index = lax.axis_index("narrow")
    me = wide_index * narrow_count + narrow_index
    peer_count = wide_count * narrow_count
    shard_rows, request_count, channels = cache_ref.shape
    slab_rows = outgoing.shape[1]
    late_source = (wide_count - 1) * narrow_count

    cache_copy = pltpu.make_async_copy(cache_hbm, cache_ref, local_sem.at[0])
    send_sem = local_sem.at[0]
    slots_copy = pltpu.make_async_copy(slots_hbm, slots_ref, local_sem.at[1])
    query_copy = pltpu.make_async_copy(query_hbm, query_ref, local_sem.at[1])
    lengths_copy = pltpu.make_async_copy(lengths_hbm, lengths_ref, local_sem.at[1])

    def device(index):
        if isinstance(index, int):
            return {"wide": index // narrow_count, "narrow": index % narrow_count}
        return {"wide": lax.div(index, narrow_count), "narrow": lax.rem(index, narrow_count)}

    def signal(semaphore, index):
        pl.semaphore_signal(
            semaphore, inc=1, device_id=device(index), device_id_type=pl.DeviceIdType.MESH
        )

    hub = narrow_count - 1
    is_hub = me == hub
    group_wides = -(-(wide_count - 1) // GROUP_LIMIT)
    group_count = -(-(wide_count - 1) // group_wides)
    group = lax.div(wide_index + group_wides - 1, group_wides) - 1
    barrier = pltpu.get_barrier_semaphore()

    @pl.when((wide_index == 0) & ~is_hub)
    def _():
        signal(barrier, hub)

    pl.semaphore_wait(barrier, jnp.where(is_hub, narrow_count - 1, 1))

    if direct:
        direct_copy = pltpu.make_async_remote_copy(
            src_ref=cache_hbm,
            dst_ref=direct_ref,
            send_sem=late_sem,
            recv_sem=late_sem,
            device_id=device(0),
            device_id_type=pl.DeviceIdType.MESH,
        )
        is_late_source = me == late_source

        @pl.when(is_late_source)
        def _():
            direct_copy.start()

    for at in range(shard_rows):
        pltpu.make_async_copy(cache_hbm.at[at], cache_ref.at[at], local_sem.at[0]).start()
    slots_copy.start()

    @pl.when(group == 0)
    def _():
        signal(barrier, hub)

    @pl.when(group > 0)
    def _():
        signal(arrived_sem.at[group - 1], hub)

    def announce():
        loop(peer_count - narrow_count, lambda step: signal(barrier, peer_count - 1 - step))
        loop(narrow_count - 1, lambda step: signal(barrier, step))

    pl.when(is_hub)(announce)

    slots_copy.wait()
    lengths_copy.start()
    slot_row = slots_ref[...].reshape(1, request_count)
    shape = (request_count * slab_rows, request_count)
    row = lax.broadcasted_iota(jnp.int32, shape, 0)
    picks = [
        (slot_row * slab_rows + offset == row).astype(jnp.float32).astype(jnp.bfloat16)
        for offset in range(shard_rows)
    ]
    cache_copy.wait()
    ordered = None
    for offset in range(shard_rows):
        term = jnp.dot(picks[offset], cache_ref[offset], preferred_element_type=jnp.float32)
        ordered = term if ordered is None else ordered + term
    outgoing[...] = ordered.astype(jnp.bfloat16).reshape(outgoing.shape)

    def send(index, target_ref, target_sem, wanted):
        target = device(index)

        @pl.when(wanted)
        def _():
            pltpu.make_async_remote_copy(
                src_ref=outgoing.at[target["wide"]],
                dst_ref=target_ref,
                send_sem=send_sem,
                recv_sem=target_sem,
                device_id=target,
                device_id_type=pl.DeviceIdType.MESH,
            ).start()

    def send_slab(index, wanted=True):
        send(index, received.at[me], recv_sem, (index != me) & wanted)

    for core in range(narrow_count):
        if direct:
            send_slab(core, ~is_late_source)
            if core > 0:
                send(core, late_ref, late_sem, is_late_source)
        else:
            send_slab(core)
    lengths_copy.wait()
    query_copy.start()
    received[me] = outgoing[wide_index]
    if direct:

        @pl.when(wide_index == 0)
        def _():
            received[late_source] = jnp.zeros(received.shape[1:], received.dtype)

    for step in range(group_count):
        first = (1 + step * group_wides) * narrow_count
        last = min(1 + (step + 1) * group_wides, wide_count) * narrow_count

        @pl.when(is_hub)
        def _():
            answered = barrier if step == 0 else arrived_sem.at[step - 1]
            pl.semaphore_wait(answered, last - first)
            announce()

        @pl.when(~is_hub)
        def _():
            pl.semaphore_wait(barrier, 1)

        loop(last - first, lambda at: send_slab(at + first))

    query_copy.wait()
    own = slot_row == wide_index
    own_length = jnp.sum(
        jnp.where(own, lengths_ref[...].reshape(1, request_count).astype(jnp.float32), 0.0),
        axis=1,
        keepdims=True,
    )
    _, forward_steps, head_count, _ = query_ref.shape
    tile_heads = math.gcd(head_count, 8)
    score_shape = (forward_steps * head_count, peer_count * slab_rows)
    query_rows = query_ref[...].reshape(score_shape[0], channels)
    column = lax.broadcasted_iota(jnp.int32, score_shape, 1)
    offset = column % slab_rows
    source = column // slab_rows
    place = source * shard_rows + offset
    token = lax.broadcasted_iota(jnp.int32, score_shape, 0) // head_count
    visible = (offset < shard_rows) & ((place - token).astype(jnp.float32) < own_length + 1.0)
    if direct:
        visible = visible & ((source != late_source) | (wide_index != 0))
        square = (request_count, request_count)
        diagonal = lax.broadcasted_iota(jnp.int32, square, 0) == lax.broadcasted_iota(
            jnp.int32, square, 1
        )
        own_column = jnp.sum(jnp.where(diagonal & own, 1.0, 0.0), axis=1, keepdims=True)
        query_wide = query_rows.astype(jnp.float32) * score_scale
        late_token = lax.broadcasted_iota(jnp.int32, (score_shape[0], 1), 0) // head_count
        late_visible = [
            (late_source * shard_rows + at - late_token).astype(jnp.float32) < own_length + 1.0
            for at in range(shard_rows)
        ]

    def wait_slabs(semaphore, one_fewer):
        def wait(count):
            slabs = received.at[pl.ds(0, count)]
            pltpu.make_async_copy(slabs, slabs, semaphore).wait()

        if direct:
            pl.when(one_fewer)(lambda: wait(peer_count - 2))
            pl.when(~one_fewer)(lambda: wait(peer_count - 1))
        else:
            wait(peer_count - 1)

    wait_slabs(recv_sem, wide_index == 0)

    keys = received[...].reshape(peer_count * slab_rows, channels)
    scores = (
        lax.dot_general(
            query_rows, keys, (((1,), (1,)), ((), ())), preferred_element_type=jnp.float32
        )
        * score_scale
    )
    scores = jnp.where(visible, scores, floor_value)
    highest = jnp.max(scores, axis=1, keepdims=True)
    weights = jnp.exp2(scores - highest)
    weight_sum = jnp.sum(weights, axis=1, keepdims=True)
    latent_total = jnp.dot(
        weights.astype(jnp.bfloat16), keys[:, :LATENT_WIDTH], preferred_element_type=jnp.float32
    )

    def finish(total, total_weight):
        out_ref[...] = (total / total_weight).astype(jnp.bfloat16).reshape(out_ref.shape)

    if direct:

        @pl.when(wide_index != 0)
        def _():
            finish(latent_total, weight_sum)

        def fold(late_rows):
            for token in range(forward_steps):
                for head in range(0, head_count, tile_heads):
                    rows = slice(token * head_count + head, token * head_count + head + tile_heads)
                    late_scores, joint = [], highest[rows]
                    for at in range(shard_rows):
                        score = jnp.sum(query_wide[rows] * late_rows[at], axis=1, keepdims=True)
                        score = jnp.where(late_visible[at][rows], score, floor_value)
                        joint = jnp.maximum(joint, score)
                        late_scores.append(score)
                    scale = jnp.exp2(highest[rows] - joint)
                    total_weight = weight_sum[rows] * scale
                    total = latent_total[rows] * scale
                    for at in range(shard_rows):
                        weight = jnp.exp2(late_scores[at] - joint)
                        total_weight = total_weight + weight
                        total = total + weight * late_rows[at][:, :LATENT_WIDTH]
                    attended = (total / total_weight).astype(jnp.bfloat16)
                    out_ref[0, token, head : head + tile_heads, :] = attended

        @pl.when(me == 0)
        def _():
            direct_copy.wait_recv()
            fold([
                jnp.sum(direct_ref[at].astype(jnp.float32) * own_column, axis=0, keepdims=True)
                for at in range(shard_rows)
            ])

        @pl.when((wide_index == 0) & (me != 0))
        def _():
            pltpu.make_async_copy(late_ref, late_ref, late_sem).wait()
            late_slab = late_ref[...].astype(jnp.float32)
            fold([late_slab[at : at + 1] for at in range(shard_rows)])
    else:
        finish(latent_total, weight_sum)
    wait_slabs(send_sem, is_late_source if direct else False)
    if direct:

        @pl.when(is_late_source)
        def _():
            direct_copy.wait_send()


def padded_bytes(rows, columns):
    return rows * -(-columns // 128) * 128 * 4


def shards(cache, lengths, slots, query):
    wide_count = lax.axis_size("wide")
    narrow_count = lax.axis_size("narrow")
    peer_count = wide_count * narrow_count
    request_count, shard_rows, channels = cache.shape
    _, forward_steps, head_count, _ = query.shape
    slab_rows = pl.next_power_of_2(shard_rows)
    direct = wide_count % 2 == 0 and request_count * shard_rows <= DIRECT_LIMIT
    group_wides = -(-(wide_count - 1) // GROUP_LIMIT)
    group_count = -(-(wide_count - 1) // group_wides)
    slabs = (request_count + peer_count) * slab_rows
    limit = (4 << 20) + 4 * padded_bytes(slabs, channels)
    return pl.pallas_call(
        functools.partial(kernel, wide_count, narrow_count, direct),
        out_shape=jax.ShapeDtypeStruct((1, forward_steps, head_count, LATENT_WIDTH), jnp.bfloat16),
        in_specs=[pl.BlockSpec(memory_space=pltpu.HBM)] * 4,
        out_specs=pl.BlockSpec(memory_space=pltpu.VMEM),
        scratch_shapes=[
            pltpu.VMEM((shard_rows, request_count, channels), cache.dtype),
            pltpu.VMEM(lengths.shape, lengths.dtype),
            pltpu.VMEM(slots.shape, slots.dtype),
            pltpu.VMEM(query.shape, query.dtype),
            pltpu.VMEM((request_count, slab_rows, channels), cache.dtype),
            pltpu.VMEM((peer_count, slab_rows, channels), cache.dtype),
            pltpu.VMEM((shard_rows, request_count, channels), cache.dtype),
            pltpu.VMEM((slab_rows, channels), cache.dtype),
            pltpu.SemaphoreType.DMA((2,)),
            pltpu.SemaphoreType.DMA,
            pltpu.SemaphoreType.DMA,
            pltpu.SemaphoreType.REGULAR((max(group_count - 1, 1),)),
        ],
        compiler_params=pltpu.CompilerParams(
            collective_id=0, has_side_effects=True, vmem_limit_bytes=limit
        ),
    )(*[
        pltpu.with_memory_space_constraint(argument, pltpu.HBM)
        for argument in (jnp.transpose(cache, (1, 0, 2)), lengths, slots, query)
    ])


def solution(mesh):
    return jax.shard_map(
        shards,
        mesh=mesh,
        in_specs=(
            P("grp", ("wide", "narrow"), None),
            P("grp"),
            P("grp"),
            P(("grp", "wide"), None, "narrow", None),
        ),
        out_specs=P(("grp", "wide"), None, "narrow", None),
        check_vma=False,
    )
```

```python
import functools
import math

import jax
import jax.numpy as jnp
from jax import lax
from jax.experimental import pallas as pl
from jax.experimental.pallas import tpu as pltpu
from jax.sharding import PartitionSpec as P

LATENT_WIDTH = 512
UNROLL_LIMIT = 16
GROUP_LIMIT = 4
DIRECT_LIMIT = 64

score_scale = 0.0721687836 * math.log2(math.e)
floor_value = -1e30


def loop(count, body):
    if count <= UNROLL_LIMIT:
        for step in range(count):
            body(step)
    else:
        lax.fori_loop(0, count, lambda step, carry: (body(step), carry)[1], 0)


def kernel(
    wide_count,
    narrow_count,
    direct,
    cache_hbm,
    lengths_hbm,
    slots_hbm,
    query_hbm,
    out_ref,
    cache_ref,
    lengths_ref,
    slots_ref,
    query_ref,
    outgoing,
    received,
    direct_ref,
    late_ref,
    local_sem,
    recv_sem,
    late_sem,
    arrived_sem,
):
    wide_index = lax.axis_index("wide")
    narrow_index = lax.axis_index("narrow")
    me = wide_index * narrow_count + narrow_index
    peer_count = wide_count * narrow_count
    shard_rows, request_count, channels = cache_ref.shape
    slab_rows = outgoing.shape[1]
    late_source = (wide_count - 1) * narrow_count

    cache_copy = pltpu.make_async_copy(cache_hbm, cache_ref, local_sem.at[0])
    send_sem = local_sem.at[0]
    slots_copy = pltpu.make_async_copy(slots_hbm, slots_ref, local_sem.at[1])
    query_copy = pltpu.make_async_copy(query_hbm, query_ref, local_sem.at[1])
    lengths_copy = pltpu.make_async_copy(lengths_hbm, lengths_ref, local_sem.at[1])

    def device(index):
        if isinstance(index, int):
            return {"wide": index // narrow_count, "narrow": index % narrow_count}
        return {"wide": lax.div(index, narrow_count), "narrow": lax.rem(index, narrow_count)}

    def signal(semaphore, index):
        pl.semaphore_signal(
            semaphore, inc=1, device_id=device(index), device_id_type=pl.DeviceIdType.MESH
        )

    hub = narrow_count - 1
    is_hub = me == hub
    group_wides = -(-(wide_count - 1) // GROUP_LIMIT)
    group_count = -(-(wide_count - 1) // group_wides)
    group = lax.div(wide_index + group_wides - 1, group_wides) - 1
    barrier = pltpu.get_barrier_semaphore()

    @pl.when((wide_index == 0) & ~is_hub)
    def _():
        signal(barrier, hub)

    pl.semaphore_wait(barrier, jnp.where(is_hub, narrow_count - 1, 1))

    if direct:
        direct_copy = pltpu.make_async_remote_copy(
            src_ref=cache_hbm,
            dst_ref=direct_ref,
            send_sem=late_sem,
            recv_sem=late_sem,
            device_id=device(0),
            device_id_type=pl.DeviceIdType.MESH,
        )
        is_late_source = me == late_source

        @pl.when(is_late_source)
        def _():
            direct_copy.start()

    cache_copy.start()
    slots_copy.start()

    @pl.when(group == 0)
    def _():
        signal(barrier, hub)

    @pl.when(group > 0)
    def _():
        signal(arrived_sem.at[group - 1], hub)

    def announce():
        loop(narrow_count - 1, lambda step: signal(barrier, step))
        loop(peer_count - narrow_count, lambda step: signal(barrier, step + narrow_count))

    pl.when(is_hub)(announce)

    slots_copy.wait()
    lengths_copy.start()
    slot_row = slots_ref[...].reshape(1, request_count)
    shape = (request_count * slab_rows, shard_rows * request_count)
    slot_tiled = jnp.concatenate([slot_row] * shard_rows, axis=1)
    row = lax.broadcasted_iota(jnp.int32, shape, 0)
    column = lax.broadcasted_iota(jnp.int32, shape, 1)
    pick = (slot_tiled * slab_rows + lax.div(column, request_count) == row).astype(jnp.float32)
    pick = pick.astype(jnp.bfloat16)
    cache_copy.wait()
    shard = cache_ref[...].reshape(shard_rows * request_count, channels)
    ordered = jnp.dot(pick, shard, preferred_element_type=jnp.float32)
    outgoing[...] = ordered.astype(jnp.bfloat16).reshape(outgoing.shape)

    def send(index, target_ref, target_sem, wanted):
        target = device(index)

        @pl.when(wanted)
        def _():
            pltpu.make_async_remote_copy(
                src_ref=outgoing.at[target["wide"]],
                dst_ref=target_ref,
                send_sem=send_sem,
                recv_sem=target_sem,
                device_id=target,
                device_id_type=pl.DeviceIdType.MESH,
            ).start()

    def send_slab(index, wanted=True):
        send(index, received.at[me], recv_sem, (index != me) & wanted)

    for core in range(narrow_count):
        if direct:
            send_slab(core, ~is_late_source)
            if core > 0:
                send(core, late_ref, late_sem, is_late_source)
        else:
            send_slab(core)
    lengths_copy.wait()
    query_copy.start()
    received[me] = outgoing[wide_index]
    if direct:

        @pl.when(wide_index == 0)
        def _():
            received[late_source] = jnp.zeros(received.shape[1:], received.dtype)

    for step in range(group_count):
        first = (1 + step * group_wides) * narrow_count
        last = min(1 + (step + 1) * group_wides, wide_count) * narrow_count

        @pl.when(is_hub)
        def _():
            answered = barrier if step == 0 else arrived_sem.at[step - 1]
            pl.semaphore_wait(answered, last - first)
            announce()

        @pl.when(~is_hub)
        def _():
            pl.semaphore_wait(barrier, 1)

        loop(last - first, lambda at: send_slab(at + first))

    query_copy.wait()
    own = slot_row == wide_index
    own_length = jnp.sum(
        jnp.where(own, lengths_ref[...].reshape(1, request_count).astype(jnp.float32), 0.0),
        axis=1,
        keepdims=True,
    )
    _, forward_steps, head_count, _ = query_ref.shape
    tile_heads = math.gcd(head_count, 8)
    score_shape = (forward_steps * head_count, peer_count * slab_rows)
    query_rows = query_ref[...].reshape(score_shape[0], channels)
    column = lax.broadcasted_iota(jnp.int32, score_shape, 1)
    offset = column % slab_rows
    source = column // slab_rows
    place = source * shard_rows + offset
    token = lax.broadcasted_iota(jnp.int32, score_shape, 0) // head_count
    visible = (offset < shard_rows) & ((place - token).astype(jnp.float32) < own_length + 1.0)
    if direct:
        visible = visible & ((source != late_source) | (wide_index != 0))
        square = (request_count, request_count)
        diagonal = lax.broadcasted_iota(jnp.int32, square, 0) == lax.broadcasted_iota(
            jnp.int32, square, 1
        )
        own_column = jnp.sum(jnp.where(diagonal & own, 1.0, 0.0), axis=1, keepdims=True)
        query_wide = query_rows.astype(jnp.float32) * score_scale
        late_token = lax.broadcasted_iota(jnp.int32, (score_shape[0], 1), 0) // head_count
        late_visible = [
            (late_source * shard_rows + at - late_token).astype(jnp.float32) < own_length + 1.0
            for at in range(shard_rows)
        ]

    def wait_slabs(semaphore, one_fewer):
        def wait(count):
            slabs = received.at[pl.ds(0, count)]
            pltpu.make_async_copy(slabs, slabs, semaphore).wait()

        if direct:
            pl.when(one_fewer)(lambda: wait(peer_count - 2))
            pl.when(~one_fewer)(lambda: wait(peer_count - 1))
        else:
            wait(peer_count - 1)

    wait_slabs(recv_sem, wide_index == 0)

    keys = received[...].reshape(peer_count * slab_rows, channels)
    scores = (
        lax.dot_general(
            query_rows, keys, (((1,), (1,)), ((), ())), preferred_element_type=jnp.float32
        )
        * score_scale
    )
    scores = jnp.where(visible, scores, floor_value)
    highest = jnp.max(scores, axis=1, keepdims=True)
    weights = jnp.exp2(scores - highest)
    weight_sum = jnp.sum(weights, axis=1, keepdims=True)
    latent_total = jnp.dot(
        weights.astype(jnp.bfloat16), keys[:, :LATENT_WIDTH], preferred_element_type=jnp.float32
    )

    def finish(total, total_weight):
        out_ref[...] = (total / total_weight).astype(jnp.bfloat16).reshape(out_ref.shape)

    if direct:

        @pl.when(wide_index != 0)
        def _():
            finish(latent_total, weight_sum)

        def fold(late_rows):
            for token in range(forward_steps):
                for head in range(0, head_count, tile_heads):
                    rows = slice(token * head_count + head, token * head_count + head + tile_heads)
                    late_scores, joint = [], highest[rows]
                    for at in range(shard_rows):
                        score = jnp.sum(query_wide[rows] * late_rows[at], axis=1, keepdims=True)
                        score = jnp.where(late_visible[at][rows], score, floor_value)
                        joint = jnp.maximum(joint, score)
                        late_scores.append(score)
                    scale = jnp.exp2(highest[rows] - joint)
                    total_weight = weight_sum[rows] * scale
                    total = latent_total[rows] * scale
                    for at in range(shard_rows):
                        weight = jnp.exp2(late_scores[at] - joint)
                        total_weight = total_weight + weight
                        total = total + weight * late_rows[at][:, :LATENT_WIDTH]
                    attended = (total / total_weight).astype(jnp.bfloat16)
                    out_ref[0, token, head : head + tile_heads, :] = attended

        @pl.when(me == 0)
        def _():
            direct_copy.wait_recv()
            fold([
                jnp.sum(direct_ref[at].astype(jnp.float32) * own_column, axis=0, keepdims=True)
                for at in range(shard_rows)
            ])

        @pl.when((wide_index == 0) & (me != 0))
        def _():
            pltpu.make_async_copy(late_ref, late_ref, late_sem).wait()
            late_slab = late_ref[...].astype(jnp.float32)
            fold([late_slab[at : at + 1] for at in range(shard_rows)])
    else:
        finish(latent_total, weight_sum)
    wait_slabs(send_sem, is_late_source if direct else False)
    if direct:

        @pl.when(is_late_source)
        def _():
            direct_copy.wait_send()


def padded_bytes(rows, columns):
    return rows * -(-columns // 128) * 128 * 4


def shards(cache, lengths, slots, query):
    wide_count = lax.axis_size("wide")
    narrow_count = lax.axis_size("narrow")
    peer_count = wide_count * narrow_count
    request_count, shard_rows, channels = cache.shape
    _, forward_steps, head_count, _ = query.shape
    slab_rows = pl.next_power_of_2(shard_rows)
    direct = wide_count % 2 == 0 and request_count * shard_rows <= DIRECT_LIMIT
    group_wides = -(-(wide_count - 1) // GROUP_LIMIT)
    group_count = -(-(wide_count - 1) // group_wides)
    slabs = (request_count + peer_count) * slab_rows
    limit = (4 << 20) + 4 * padded_bytes(slabs, channels)
    return pl.pallas_call(
        functools.partial(kernel, wide_count, narrow_count, direct),
        out_shape=jax.ShapeDtypeStruct((1, forward_steps, head_count, LATENT_WIDTH), jnp.bfloat16),
        in_specs=[pl.BlockSpec(memory_space=pltpu.HBM)] * 4,
        out_specs=pl.BlockSpec(memory_space=pltpu.VMEM),
        scratch_shapes=[
            pltpu.VMEM((shard_rows, request_count, channels), cache.dtype),
            pltpu.VMEM(lengths.shape, lengths.dtype),
            pltpu.VMEM(slots.shape, slots.dtype),
            pltpu.VMEM(query.shape, query.dtype),
            pltpu.VMEM((request_count, slab_rows, channels), cache.dtype),
            pltpu.VMEM((peer_count, slab_rows, channels), cache.dtype),
            pltpu.VMEM((shard_rows, request_count, channels), cache.dtype),
            pltpu.VMEM((slab_rows, channels), cache.dtype),
            pltpu.SemaphoreType.DMA((2,)),
            pltpu.SemaphoreType.DMA,
            pltpu.SemaphoreType.DMA,
            pltpu.SemaphoreType.REGULAR((max(group_count - 1, 1),)),
        ],
        compiler_params=pltpu.CompilerParams(
            collective_id=0, has_side_effects=True, vmem_limit_bytes=limit
        ),
    )(*[
        pltpu.with_memory_space_constraint(argument, pltpu.HBM)
        for argument in (jnp.transpose(cache, (1, 0, 2)), lengths, slots, query)
    ])


def solution(mesh):
    return jax.shard_map(
        shards,
        mesh=mesh,
        in_specs=(
            P("grp", ("wide", "narrow"), None),
            P("grp"),
            P("grp"),
            P(("grp", "wide"), None, "narrow", None),
        ),
        out_specs=P(("grp", "wide"), None, "narrow", None),
        check_vma=False,
    )
```

```python
import functools
import math

import jax
import jax.numpy as jnp
from jax import lax
from jax.experimental import pallas as pl
from jax.experimental.pallas import tpu as pltpu
from jax.sharding import PartitionSpec as P

LATENT_WIDTH = 512
UNROLL_LIMIT = 16
GROUP_LIMIT = 4
DIRECT_LIMIT = 64

score_scale = 0.0721687836 * math.log2(math.e)
floor_value = -1e30


def loop(count, body):
    if count <= UNROLL_LIMIT:
        for step in range(count):
            body(step)
    else:
        lax.fori_loop(0, count, lambda step, carry: (body(step), carry)[1], 0)


def kernel(
    wide_count,
    narrow_count,
    direct,
    cache_hbm,
    lengths_hbm,
    slots_hbm,
    query_hbm,
    out_ref,
    cache_ref,
    lengths_ref,
    slots_ref,
    query_ref,
    outgoing,
    received,
    direct_ref,
    late_ref,
    local_sem,
    recv_sem,
    late_sem,
    arrived_sem,
):
    wide_index = lax.axis_index("wide")
    narrow_index = lax.axis_index("narrow")
    me = wide_index * narrow_count + narrow_index
    peer_count = wide_count * narrow_count
    shard_rows, request_count, channels = cache_ref.shape
    slab_rows = outgoing.shape[1]
    late_source = (wide_count - 1) * narrow_count

    cache_copy = pltpu.make_async_copy(cache_hbm, cache_ref, local_sem.at[0])
    send_sem = local_sem.at[0]
    slots_copy = pltpu.make_async_copy(slots_hbm, slots_ref, local_sem.at[1])
    query_copy = pltpu.make_async_copy(query_hbm, query_ref, local_sem.at[1])
    lengths_copy = pltpu.make_async_copy(lengths_hbm, lengths_ref, local_sem.at[1])

    def device(index):
        if isinstance(index, int):
            return {"wide": index // narrow_count, "narrow": index % narrow_count}
        return {"wide": lax.div(index, narrow_count), "narrow": lax.rem(index, narrow_count)}

    def signal(semaphore, index):
        pl.semaphore_signal(
            semaphore, inc=1, device_id=device(index), device_id_type=pl.DeviceIdType.MESH
        )

    hub = narrow_count - 1
    is_hub = me == hub
    group_wides = -(-(wide_count - 1) // GROUP_LIMIT)
    group_count = -(-(wide_count - 1) // group_wides)
    group = lax.div(wide_index + group_wides - 1, group_wides) - 1
    barrier = pltpu.get_barrier_semaphore()

    @pl.when((wide_index == 0) & ~is_hub)
    def _():
        signal(barrier, hub)

    pl.semaphore_wait(barrier, jnp.where(is_hub, narrow_count - 1, 1))

    if direct:
        direct_copy = pltpu.make_async_remote_copy(
            src_ref=cache_hbm,
            dst_ref=direct_ref,
            send_sem=late_sem,
            recv_sem=late_sem,
            device_id=device(0),
            device_id_type=pl.DeviceIdType.MESH,
        )
        is_late_source = me == late_source

        @pl.when(is_late_source)
        def _():
            direct_copy.start()

    for at in range(shard_rows):
        pltpu.make_async_copy(cache_hbm.at[at], cache_ref.at[at], local_sem.at[0]).start()
    slots_copy.start()

    @pl.when(group == 0)
    def _():
        signal(barrier, hub)

    @pl.when(group > 0)
    def _():
        signal(arrived_sem.at[group - 1], hub)

    def announce():
        loop(narrow_count - 1, lambda step: signal(barrier, step))
        loop(peer_count - narrow_count, lambda step: signal(barrier, step + narrow_count))

    pl.when(is_hub)(announce)

    slots_copy.wait()
    lengths_copy.start()
    slot_row = slots_ref[...].reshape(1, request_count)
    shape = (request_count * slab_rows, request_count)
    row = lax.broadcasted_iota(jnp.int32, shape, 0)
    picks = [
        (slot_row * slab_rows + offset == row).astype(jnp.float32).astype(jnp.bfloat16)
        for offset in range(shard_rows)
    ]
    cache_copy.wait()
    ordered = None
    for offset in range(shard_rows):
        term = jnp.dot(picks[offset], cache_ref[offset], preferred_element_type=jnp.float32)
        ordered = term if ordered is None else ordered + term
    outgoing[...] = ordered.astype(jnp.bfloat16).reshape(outgoing.shape)

    def send(index, target_ref, target_sem, wanted):
        target = device(index)

        @pl.when(wanted)
        def _():
            pltpu.make_async_remote_copy(
                src_ref=outgoing.at[target["wide"]],
                dst_ref=target_ref,
                send_sem=send_sem,
                recv_sem=target_sem,
                device_id=target,
                device_id_type=pl.DeviceIdType.MESH,
            ).start()

    def send_slab(index, wanted=True):
        send(index, received.at[me], recv_sem, (index != me) & wanted)

    for core in range(narrow_count):
        if direct:
            send_slab(core, ~is_late_source)
            if core > 0:
                send(core, late_ref, late_sem, is_late_source)
        else:
            send_slab(core)
    lengths_copy.wait()
    query_copy.start()
    received[me] = outgoing[wide_index]
    if direct:

        @pl.when(wide_index == 0)
        def _():
            received[late_source] = jnp.zeros(received.shape[1:], received.dtype)

    for step in range(group_count):
        first = (1 + step * group_wides) * narrow_count
        last = min(1 + (step + 1) * group_wides, wide_count) * narrow_count

        @pl.when(is_hub)
        def _():
            answered = barrier if step == 0 else arrived_sem.at[step - 1]
            pl.semaphore_wait(answered, last - first)
            announce()

        @pl.when(~is_hub)
        def _():
            pl.semaphore_wait(barrier, 1)

        loop(last - first, lambda at: send_slab(at + first))

    query_copy.wait()
    own = slot_row == wide_index
    own_length = jnp.sum(
        jnp.where(own, lengths_ref[...].reshape(1, request_count).astype(jnp.float32), 0.0),
        axis=1,
        keepdims=True,
    )
    _, forward_steps, head_count, _ = query_ref.shape
    tile_heads = math.gcd(head_count, 8)
    score_shape = (forward_steps * head_count, peer_count * slab_rows)
    query_rows = query_ref[...].reshape(score_shape[0], channels)
    column = lax.broadcasted_iota(jnp.int32, score_shape, 1)
    offset = column % slab_rows
    source = column // slab_rows
    place = source * shard_rows + offset
    token = lax.broadcasted_iota(jnp.int32, score_shape, 0) // head_count
    visible = (offset < shard_rows) & ((place - token).astype(jnp.float32) < own_length + 1.0)
    if direct:
        visible = visible & ((source != late_source) | (wide_index != 0))
        square = (request_count, request_count)
        diagonal = lax.broadcasted_iota(jnp.int32, square, 0) == lax.broadcasted_iota(
            jnp.int32, square, 1
        )
        own_column = jnp.sum(jnp.where(diagonal & own, 1.0, 0.0), axis=1, keepdims=True)
        query_wide = query_rows.astype(jnp.float32) * score_scale
        late_token = lax.broadcasted_iota(jnp.int32, (score_shape[0], 1), 0) // head_count
        late_visible = [
            (late_source * shard_rows + at - late_token).astype(jnp.float32) < own_length + 1.0
            for at in range(shard_rows)
        ]

    def wait_slabs(semaphore, one_fewer):
        def wait(count):
            slabs = received.at[pl.ds(0, count)]
            pltpu.make_async_copy(slabs, slabs, semaphore).wait()

        if direct:
            pl.when(one_fewer)(lambda: wait(peer_count - 2))
            pl.when(~one_fewer)(lambda: wait(peer_count - 1))
        else:
            wait(peer_count - 1)

    wait_slabs(recv_sem, wide_index == 0)

    keys = received[...].reshape(peer_count * slab_rows, channels)
    scores = (
        lax.dot_general(
            query_rows, keys, (((1,), (1,)), ((), ())), preferred_element_type=jnp.float32
        )
        * score_scale
    )
    scores = jnp.where(visible, scores, floor_value)
    highest = jnp.max(scores, axis=1, keepdims=True)
    weights = jnp.exp2(scores - highest)
    weight_sum = jnp.sum(weights, axis=1, keepdims=True)
    latent_total = jnp.dot(
        weights.astype(jnp.bfloat16), keys[:, :LATENT_WIDTH], preferred_element_type=jnp.float32
    )

    def finish(total, total_weight):
        out_ref[...] = (total / total_weight).astype(jnp.bfloat16).reshape(out_ref.shape)

    if direct:

        @pl.when(wide_index != 0)
        def _():
            finish(latent_total, weight_sum)

        def fold(late_rows):
            for token in range(forward_steps):
                for head in range(0, head_count, tile_heads):
                    rows = slice(token * head_count + head, token * head_count + head + tile_heads)
                    late_scores, joint = [], highest[rows]
                    for at in range(shard_rows):
                        score = jnp.sum(query_wide[rows] * late_rows[at], axis=1, keepdims=True)
                        score = jnp.where(late_visible[at][rows], score, floor_value)
                        joint = jnp.maximum(joint, score)
                        late_scores.append(score)
                    scale = jnp.exp2(highest[rows] - joint)
                    total_weight = weight_sum[rows] * scale
                    total = latent_total[rows] * scale
                    for at in range(shard_rows):
                        weight = jnp.exp2(late_scores[at] - joint)
                        total_weight = total_weight + weight
                        total = total + weight * late_rows[at][:, :LATENT_WIDTH]
                    attended = (total / total_weight).astype(jnp.bfloat16)
                    out_ref[0, token, head : head + tile_heads, :] = attended

        @pl.when(me == 0)
        def _():
            direct_copy.wait_recv()
            fold([
                jnp.sum(direct_ref[at].astype(jnp.float32) * own_column, axis=0, keepdims=True)
                for at in range(shard_rows)
            ])

        @pl.when((wide_index == 0) & (me != 0))
        def _():
            pltpu.make_async_copy(late_ref, late_ref, late_sem).wait()
            late_slab = late_ref[...].astype(jnp.float32)
            fold([late_slab[at : at + 1] for at in range(shard_rows)])
    else:
        finish(latent_total, weight_sum)
    wait_slabs(send_sem, is_late_source if direct else False)
    if direct:

        @pl.when(is_late_source)
        def _():
            direct_copy.wait_send()


def padded_bytes(rows, columns):
    return rows * -(-columns // 128) * 128 * 4


def shards(cache, lengths, slots, query):
    wide_count = lax.axis_size("wide")
    narrow_count = lax.axis_size("narrow")
    peer_count = wide_count * narrow_count
    request_count, shard_rows, channels = cache.shape
    _, forward_steps, head_count, _ = query.shape
    slab_rows = pl.next_power_of_2(shard_rows)
    direct = wide_count % 2 == 0 and request_count * shard_rows <= DIRECT_LIMIT
    group_wides = -(-(wide_count - 1) // GROUP_LIMIT)
    group_count = -(-(wide_count - 1) // group_wides)
    slabs = (request_count + peer_count) * slab_rows
    limit = (4 << 20) + 4 * padded_bytes(slabs, channels)
    return pl.pallas_call(
        functools.partial(kernel, wide_count, narrow_count, direct),
        out_shape=jax.ShapeDtypeStruct((1, forward_steps, head_count, LATENT_WIDTH), jnp.bfloat16),
        in_specs=[pl.BlockSpec(memory_space=pltpu.HBM)] * 4,
        out_specs=pl.BlockSpec(memory_space=pltpu.VMEM),
        scratch_shapes=[
            pltpu.VMEM((shard_rows, request_count, channels), cache.dtype),
            pltpu.VMEM(lengths.shape, lengths.dtype),
            pltpu.VMEM(slots.shape, slots.dtype),
            pltpu.VMEM(query.shape, query.dtype),
            pltpu.VMEM((request_count, slab_rows, channels), cache.dtype),
            pltpu.VMEM((peer_count, slab_rows, channels), cache.dtype),
            pltpu.VMEM((shard_rows, request_count, channels), cache.dtype),
            pltpu.VMEM((slab_rows, channels), cache.dtype),
            pltpu.SemaphoreType.DMA((2,)),
            pltpu.SemaphoreType.DMA,
            pltpu.SemaphoreType.DMA,
            pltpu.SemaphoreType.REGULAR((max(group_count - 1, 1),)),
        ],
        compiler_params=pltpu.CompilerParams(
            collective_id=0, has_side_effects=True, vmem_limit_bytes=limit
        ),
    )(*[
        pltpu.with_memory_space_constraint(argument, pltpu.HBM)
        for argument in (jnp.transpose(cache, (1, 0, 2)), lengths, slots, query)
    ])


def solution(mesh):
    return jax.shard_map(
        shards,
        mesh=mesh,
        in_specs=(
            P("grp", ("wide", "narrow"), None),
            P("grp"),
            P("grp"),
            P(("grp", "wide"), None, "narrow", None),
        ),
        out_specs=P(("grp", "wide"), None, "narrow", None),
        check_vma=False,
    )
```

```python
import functools
import math

import jax
import jax.numpy as jnp
from jax import lax
from jax.experimental import pallas as pl
from jax.experimental.pallas import tpu as pltpu
from jax.sharding import PartitionSpec as P

LATENT_WIDTH = 512
UNROLL_LIMIT = 16
GROUP_LIMIT = 4
DIRECT_LIMIT = 64

score_scale = 0.0721687836 * math.log2(math.e)
floor_value = -1e30


def loop(count, body):
    if count <= UNROLL_LIMIT:
        for step in range(count):
            body(step)
    else:
        lax.fori_loop(0, count, lambda step, carry: (body(step), carry)[1], 0)


def kernel(
    wide_count,
    narrow_count,
    direct,
    cache_hbm,
    lengths_hbm,
    slots_hbm,
    query_hbm,
    out_ref,
    cache_ref,
    lengths_ref,
    slots_ref,
    query_ref,
    outgoing,
    received,
    direct_ref,
    late_ref,
    local_sem,
    recv_sem,
    late_sem,
    arrived_sem,
):
    wide_index = lax.axis_index("wide")
    narrow_index = lax.axis_index("narrow")
    me = wide_index * narrow_count + narrow_index
    peer_count = wide_count * narrow_count
    shard_rows, request_count, channels = cache_ref.shape
    slab_rows = outgoing.shape[1]
    late_source = (wide_count - 1) * narrow_count

    cache_copy = pltpu.make_async_copy(cache_hbm, cache_ref, local_sem.at[0])
    send_sem = local_sem.at[0]
    slots_copy = pltpu.make_async_copy(slots_hbm, slots_ref, local_sem.at[1])
    query_copy = pltpu.make_async_copy(query_hbm, query_ref, local_sem.at[1])
    lengths_copy = pltpu.make_async_copy(lengths_hbm, lengths_ref, local_sem.at[1])

    def device(index):
        if isinstance(index, int):
            return {"wide": index // narrow_count, "narrow": index % narrow_count}
        return {"wide": lax.div(index, narrow_count), "narrow": lax.rem(index, narrow_count)}

    def signal(semaphore, index):
        pl.semaphore_signal(
            semaphore, inc=1, device_id=device(index), device_id_type=pl.DeviceIdType.MESH
        )

    hub = narrow_count - 1
    is_hub = me == hub
    group_wides = -(-(wide_count - 1) // GROUP_LIMIT)
    group_count = -(-(wide_count - 1) // group_wides)
    group = lax.div(wide_index + group_wides - 1, group_wides) - 1
    barrier = pltpu.get_barrier_semaphore()

    @pl.when((wide_index == 0) & ~is_hub)
    def _():
        signal(barrier, hub)

    pl.semaphore_wait(barrier, jnp.where(is_hub, narrow_count - 1, 1))

    if direct:
        direct_copy = pltpu.make_async_remote_copy(
            src_ref=cache_hbm,
            dst_ref=direct_ref,
            send_sem=late_sem,
            recv_sem=late_sem,
            device_id=device(0),
            device_id_type=pl.DeviceIdType.MESH,
        )
        is_late_source = me == late_source

        @pl.when(is_late_source)
        def _():
            direct_copy.start()

    cache_copy.start()
    slots_copy.start()

    @pl.when(group == 0)
    def _():
        signal(barrier, hub)

    @pl.when(group > 0)
    def _():
        signal(arrived_sem.at[group - 1], hub)

    def announce():
        loop(narrow_count - 1, lambda step: signal(barrier, step))
        loop(peer_count - narrow_count, lambda step: signal(barrier, step + narrow_count))

    pl.when(is_hub)(announce)

    slots_copy.wait()
    lengths_copy.start()
    slot_row = slots_ref[...].reshape(1, request_count)
    shape = (request_count * slab_rows, shard_rows * request_count)
    slot_tiled = jnp.concatenate([slot_row] * shard_rows, axis=1)
    row = lax.broadcasted_iota(jnp.int32, shape, 0)
    column = lax.broadcasted_iota(jnp.int32, shape, 1)
    pick = (slot_tiled * slab_rows + lax.div(column, request_count) == row).astype(jnp.float32)
    pick = pick.astype(jnp.bfloat16)
    cache_copy.wait()
    shard = cache_ref[...].reshape(shard_rows * request_count, channels)
    ordered = jnp.dot(pick, shard, preferred_element_type=jnp.float32)
    outgoing[...] = ordered.astype(jnp.bfloat16).reshape(outgoing.shape)

    def send(index, target_ref, target_sem, wanted):
        target = device(index)

        @pl.when(wanted)
        def _():
            pltpu.make_async_remote_copy(
                src_ref=outgoing.at[target["wide"]],
                dst_ref=target_ref,
                send_sem=send_sem,
                recv_sem=target_sem,
                device_id=target,
                device_id_type=pl.DeviceIdType.MESH,
            ).start()

    def send_slab(index, wanted=True):
        send(index, received.at[me], recv_sem, (index != me) & wanted)

    for core in range(narrow_count):
        if direct:
            send_slab(core, ~is_late_source)
            if core > 0:
                send(core, late_ref, late_sem, is_late_source)
        else:
            send_slab(core)
    lengths_copy.wait()
    query_copy.start()
    received[me] = outgoing[wide_index]
    if direct:

        @pl.when(wide_index == 0)
        def _():
            received[late_source] = jnp.zeros(received.shape[1:], received.dtype)

    for step in range(group_count):
        first = (1 + step * group_wides) * narrow_count
        last = min(1 + (step + 1) * group_wides, wide_count) * narrow_count

        @pl.when(is_hub)
        def _():
            answered = barrier if step == 0 else arrived_sem.at[step - 1]
            pl.semaphore_wait(answered, last - first)
            announce()

        @pl.when(~is_hub)
        def _():
            pl.semaphore_wait(barrier, 1)

        loop(last - first, lambda at: send_slab(last - 1 - at))

    query_copy.wait()
    own = slot_row == wide_index
    own_length = jnp.sum(
        jnp.where(own, lengths_ref[...].reshape(1, request_count).astype(jnp.float32), 0.0),
        axis=1,
        keepdims=True,
    )
    _, forward_steps, head_count, _ = query_ref.shape
    tile_heads = math.gcd(head_count, 8)
    score_shape = (forward_steps * head_count, peer_count * slab_rows)
    query_rows = query_ref[...].reshape(score_shape[0], channels)
    column = lax.broadcasted_iota(jnp.int32, score_shape, 1)
    offset = column % slab_rows
    source = column // slab_rows
    place = source * shard_rows + offset
    token = lax.broadcasted_iota(jnp.int32, score_shape, 0) // head_count
    visible = (offset < shard_rows) & ((place - token).astype(jnp.float32) < own_length + 1.0)
    if direct:
        visible = visible & ((source != late_source) | (wide_index != 0))
        square = (request_count, request_count)
        diagonal = lax.broadcasted_iota(jnp.int32, square, 0) == lax.broadcasted_iota(
            jnp.int32, square, 1
        )
        own_column = jnp.sum(jnp.where(diagonal & own, 1.0, 0.0), axis=1, keepdims=True)
        query_wide = query_rows.astype(jnp.float32) * score_scale
        late_token = lax.broadcasted_iota(jnp.int32, (score_shape[0], 1), 0) // head_count
        late_visible = [
            (late_source * shard_rows + at - late_token).astype(jnp.float32) < own_length + 1.0
            for at in range(shard_rows)
        ]

    def wait_slabs(semaphore, one_fewer):
        def wait(count):
            slabs = received.at[pl.ds(0, count)]
            pltpu.make_async_copy(slabs, slabs, semaphore).wait()

        if direct:
            pl.when(one_fewer)(lambda: wait(peer_count - 2))
            pl.when(~one_fewer)(lambda: wait(peer_count - 1))
        else:
            wait(peer_count - 1)

    wait_slabs(recv_sem, wide_index == 0)

    keys = received[...].reshape(peer_count * slab_rows, channels)
    scores = (
        lax.dot_general(
            query_rows, keys, (((1,), (1,)), ((), ())), preferred_element_type=jnp.float32
        )
        * score_scale
    )
    scores = jnp.where(visible, scores, floor_value)
    highest = jnp.max(scores, axis=1, keepdims=True)
    weights = jnp.exp2(scores - highest)
    weight_sum = jnp.sum(weights, axis=1, keepdims=True)
    latent_total = jnp.dot(
        weights.astype(jnp.bfloat16), keys[:, :LATENT_WIDTH], preferred_element_type=jnp.float32
    )

    def finish(total, total_weight):
        out_ref[...] = (total / total_weight).astype(jnp.bfloat16).reshape(out_ref.shape)

    if direct:

        @pl.when(wide_index != 0)
        def _():
            finish(latent_total, weight_sum)

        def fold(late_rows):
            for token in range(forward_steps):
                for head in range(0, head_count, tile_heads):
                    rows = slice(token * head_count + head, token * head_count + head + tile_heads)
                    late_scores, joint = [], highest[rows]
                    for at in range(shard_rows):
                        score = jnp.sum(query_wide[rows] * late_rows[at], axis=1, keepdims=True)
                        score = jnp.where(late_visible[at][rows], score, floor_value)
                        joint = jnp.maximum(joint, score)
                        late_scores.append(score)
                    scale = jnp.exp2(highest[rows] - joint)
                    total_weight = weight_sum[rows] * scale
                    total = latent_total[rows] * scale
                    for at in range(shard_rows):
                        weight = jnp.exp2(late_scores[at] - joint)
                        total_weight = total_weight + weight
                        total = total + weight * late_rows[at][:, :LATENT_WIDTH]
                    attended = (total / total_weight).astype(jnp.bfloat16)
                    out_ref[0, token, head : head + tile_heads, :] = attended

        @pl.when(me == 0)
        def _():
            direct_copy.wait_recv()
            fold([
                jnp.sum(direct_ref[at].astype(jnp.float32) * own_column, axis=0, keepdims=True)
                for at in range(shard_rows)
            ])

        @pl.when((wide_index == 0) & (me != 0))
        def _():
            pltpu.make_async_copy(late_ref, late_ref, late_sem).wait()
            late_slab = late_ref[...].astype(jnp.float32)
            fold([late_slab[at : at + 1] for at in range(shard_rows)])
    else:
        finish(latent_total, weight_sum)
    wait_slabs(send_sem, is_late_source if direct else False)
    if direct:

        @pl.when(is_late_source)
        def _():
            direct_copy.wait_send()


def padded_bytes(rows, columns):
    return rows * -(-columns // 128) * 128 * 4


def shards(cache, lengths, slots, query):
    wide_count = lax.axis_size("wide")
    narrow_count = lax.axis_size("narrow")
    peer_count = wide_count * narrow_count
    request_count, shard_rows, channels = cache.shape
    _, forward_steps, head_count, _ = query.shape
    slab_rows = pl.next_power_of_2(shard_rows)
    direct = wide_count % 2 == 0 and request_count * shard_rows <= DIRECT_LIMIT
    group_wides = -(-(wide_count - 1) // GROUP_LIMIT)
    group_count = -(-(wide_count - 1) // group_wides)
    slabs = (request_count + peer_count) * slab_rows
    limit = (4 << 20) + 4 * padded_bytes(slabs, channels)
    return pl.pallas_call(
        functools.partial(kernel, wide_count, narrow_count, direct),
        out_shape=jax.ShapeDtypeStruct((1, forward_steps, head_count, LATENT_WIDTH), jnp.bfloat16),
        in_specs=[pl.BlockSpec(memory_space=pltpu.HBM)] * 4,
        out_specs=pl.BlockSpec(memory_space=pltpu.VMEM),
        scratch_shapes=[
            pltpu.VMEM((shard_rows, request_count, channels), cache.dtype),
            pltpu.VMEM(lengths.shape, lengths.dtype),
            pltpu.VMEM(slots.shape, slots.dtype),
            pltpu.VMEM(query.shape, query.dtype),
            pltpu.VMEM((request_count, slab_rows, channels), cache.dtype),
            pltpu.VMEM((peer_count, slab_rows, channels), cache.dtype),
            pltpu.VMEM((shard_rows, request_count, channels), cache.dtype),
            pltpu.VMEM((slab_rows, channels), cache.dtype),
            pltpu.SemaphoreType.DMA((2,)),
            pltpu.SemaphoreType.DMA,
            pltpu.SemaphoreType.DMA,
            pltpu.SemaphoreType.REGULAR((max(group_count - 1, 1),)),
        ],
        compiler_params=pltpu.CompilerParams(
            collective_id=0, has_side_effects=True, vmem_limit_bytes=limit
        ),
    )(*[
        pltpu.with_memory_space_constraint(argument, pltpu.HBM)
        for argument in (jnp.transpose(cache, (1, 0, 2)), lengths, slots, query)
    ])


def solution(mesh):
    return jax.shard_map(
        shards,
        mesh=mesh,
        in_specs=(
            P("grp", ("wide", "narrow"), None),
            P("grp"),
            P("grp"),
            P(("grp", "wide"), None, "narrow", None),
        ),
        out_specs=P(("grp", "wide"), None, "narrow", None),
        check_vma=False,
    )
```
